32 devices in a mesh: gx: 8 (over z, x), gz: 4 (over y, core).
Axes of the slice: x: 2, y: 2, z: 4, core: 2. Of those that a mesh axis runs over, the one named last changes fastest.
Arguments:
- velocity: float32 [3, 64, 128, 384], P(None, 'gx', 'gz'), may hold values from -6 to 6
- y_gap: float32 [385], replicated, may hold values from 0.2 to 2
Outputs:
- eddy_visc: float32 [64, 128, 384], P('gx', 'gz')
- lm_field: float32 [64, 128, 384], P('gx', 'gz')
- mm_field: float32 [64, 128, 384], P('gx', 'gz')
- coefficient: float32 [384], replicated
The draws below stay inside these ranges and needn't reach their ends.
All inputs are finite; a program needn't handle non-finite values.
Results may differ from the reference program's by a relative error of at most 0.00002.
Values sent between devices are 32-bit elements; how exact they have to be, the bound alone decides.
A program may use at most 64 MiB of HBM per device.

```python
import math
import jax
import jax.numpy as jnp
from jax import lax

NY = 384
NX = 64
NZ = 128


def block_levels(key, shape, split, smallest, top_value):
    gain, own = 1.0, jax.random.fold_in(key, 6)
    for dim, shards_of in split:
        draws = jnp.exp(jax.random.uniform(jax.random.fold_in(own, dim), (shards_of,), jnp.float32, smallest / len(split), top_value / len(split)))
        gain = gain * jnp.repeat(draws, shape[dim] // shards_of).reshape([-1 if axis == dim else 1 for axis in range(len(shape))])
    return gain


def scatter_about(stream_key, extent, spread, bound, cuts=(), held_as=jnp.bfloat16):
    entries = spread * jax.random.normal(stream_key, extent, jnp.float32)
    if cuts:
        entries = entries * block_levels(stream_key, extent, cuts, -0.22, 0.18)
    return jnp.clip(entries, -bound, bound).astype(held_as)


def setup_inputs(seed: int = 0) -> dict:
    arg_keys = jax.random.split(jax.random.key(seed), 3)
    velocity = scatter_about(arg_keys[0], (3, NX, NZ, NY), 1.0, 6.0, ((1, 8), (2, 4)), jnp.float32)
    y_gap = jnp.clip(jnp.exp(jax.random.uniform(arg_keys[1], (NY + 1,), jnp.float32, math.log(0.2), math.log(2.0))), 0.2, 2.0)
    return dict(velocity=velocity, y_gap=y_gap)


WEIGHTS = (1.0, 1.0, 1.0, 2.0, 2.0, 2.0)

def wall_slope(values, y_gap):
    padded = jnp.pad(values, [(0, 0)] * (values.ndim - 1) + [(1, 1)])
    return (padded[..., 2:] - padded[..., :-2]) / (y_gap[:-1] + y_gap[1:])

def strain_parts(slope_x, slope_y, slope_z):
    return jnp.stack([slope_x[0], slope_y[1], slope_z[2], 0.5 * (slope_y[0] + slope_x[1]), 0.5 * (slope_z[0] + slope_x[2]), 0.5 * (slope_z[1] + slope_y[2])])

def contract(first_part, second_part):
    summed = first_part[0] * second_part[0]
    for component in range(1, 6):
        summed = summed + WEIGHTS[component] * first_part[component] * second_part[component]
    return summed

def magnitude(strain):
    return jnp.sqrt(2.0 * contract(strain, strain))

def pair_products(speeds):
    return jnp.stack([speeds[0] * speeds[0], speeds[1] * speeds[1], speeds[2] * speeds[2], speeds[0] * speeds[1], speeds[0] * speeds[2], speeds[1] * speeds[2]])

def width_square(y_gap):
    return (0.5 * (y_gap[:-1] + y_gap[1:])) ** (2.0 / 3.0)

def germano(smooth_velocity, smooth_pairs, smooth_stress, test_strain, width_sq):
    leonard = smooth_pairs - pair_products(smooth_velocity)
    model_term = 2.0 * width_sq * (smooth_stress - 4.0 * magnitude(test_strain) * test_strain)
    return (contract(leonard, model_term), contract(model_term, model_term))

def periodic_strain(speeds, y_gap):
    slope_x = (jnp.roll(speeds, -1, 1) - jnp.roll(speeds, 1, 1)) * 0.5
    slope_z = (jnp.roll(speeds, -1, 2) - jnp.roll(speeds, 1, 2)) * 0.5
    slope_y = wall_slope(speeds, y_gap)
    return strain_parts(slope_x, slope_y, slope_z)

def periodic_filter(values):
    along_x = 0.25 * jnp.roll(values, 1, 1) + 0.5 * values + 0.25 * jnp.roll(values, -1, 1)
    return 0.25 * jnp.roll(along_x, 1, 2) + 0.5 * along_x + 0.25 * jnp.roll(along_x, -1, 2)

def reference(velocity, y_gap):
    width_sq = width_square(y_gap)
    strain = periodic_strain(velocity, y_gap)
    strain_size = magnitude(strain)
    smooth_velocity = periodic_filter(velocity)
    smooth_pairs = periodic_filter(pair_products(velocity))
    smooth_stress = periodic_filter(strain_size * strain)
    test_strain = periodic_strain(smooth_velocity, y_gap)
    lm_field, mm_field = germano(smooth_velocity, smooth_pairs, smooth_stress, test_strain, width_sq)
    planes = NX * NZ
    numerator = lax.optimization_barrier(jnp.sum(lm_field, axis=(0, 1)))
    denominator = lax.optimization_barrier(jnp.sum(mm_field, axis=(0, 1)))
    coefficient = numerator / planes / (denominator / planes + 1e-06)
    eddy_visc = coefficient * width_sq * strain_size
    return (eddy_visc, lm_field, mm_field, coefficient)
```

```python
import functools

import jax
import jax.numpy as jnp
from jax import lax
from jax.experimental import pallas as pl
from jax.experimental.pallas import tpu as pltpu
from jax.sharding import PartitionSpec as P

MESH = pl.DeviceIdType.MESH
LANES = 128
RIM = 8
DIRECT = 64


def width_square(span):
    return jnp.exp(jnp.log(0.5 * span) * (2.0 / 3.0))


def finish(size_ref, lm_ref, mm_ref, coef_ref, eddy_out, lm_out, mm_out, coef_out, eddy_s, sem):
    nx, _, ny = size_ref.shape
    copies = [pltpu.make_async_copy(lm_ref, lm_out, sem.at[0]), pltpu.make_async_copy(mm_ref, mm_out, sem.at[1])]
    for copy in copies:
        copy.start()
    factor = coef_ref[1:2]
    for r in range(0, nx, 2):
        rows = pl.ds(r, 2)
        eddy_s[rows] = factor * size_ref[rows]
        copy = pltpu.make_async_copy(eddy_s.at[rows], eddy_out.at[rows], sem.at[2 + r // 2])
        copy.start()
        copies.append(copy)
    coef_out[...] = coef_ref[0:1].reshape(ny)
    for copy in copies:
        copy.wait()


def doublings(size):
    reach, steps = 1, []
    while reach < size // 2:
        steps.append(reach)
        reach *= 2
    return steps


def kernel(gxn, gzn, cells, gap_hbm, vel_ref, size_s, lm_s, mm_s, out_coef_ref,
           pad, zvel, zpair, zstress, slope, tslope, vslope, coef_ref, sums, accs,
           gap_ref, gap_sem, load_sem, xs_sem, xr_sem, ks_sem, kr_sem, cs_sem, cr_sem,
           near_x, near_z, near_all, as_sem, ar_sem):
    gx, gz = lax.axis_index("gx"), lax.axis_index("gz")
    nx, nz, ny = vel_ref.shape[1:]
    wide = nz + RIM
    tiles = [pl.ds(t, LANES) for t in range(0, ny, LANES)]

    def along_x(d):
        return (lax.rem(gx + d + gxn, gxn), gz)

    def along_z(d):
        return (gx, lax.rem(gz + d + gzn, gzn))

    def signal(sem, device):
        pl.semaphore_signal(sem, inc=1, device_id=device, device_id_type=MESH)

    def remote(src, dst, send, recv, device):
        return pltpu.make_async_remote_copy(
            src_ref=src, dst_ref=dst, send_sem=send, recv_sem=recv,
            device_id=device, device_id_type=MESH)

    barrier = pltpu.get_barrier_semaphore()
    for device in (along_x(1), along_x(-1), along_z(1), along_z(-1)):
        signal(barrier, device)
    loads = []
    for n, (lo, hi) in enumerate(((0, 2), (nx - 2, nx), (2, nx - 2))):
        loads.append(pltpu.make_async_copy(vel_ref.at[:, lo:hi], pad.at[:, lo + 2:hi + 2, 0:nz], load_sem.at[n]))
    for load in loads:
        load.start()
    gap_load = pltpu.make_async_copy(gap_hbm, gap_ref, gap_sem)
    gap_load.start()

    def side_rows(side):
        def pick(low, high):
            return lax.select(side == 0, low, high)
        return dict(
            inner=pick(3, nx), edge=pick(2, nx + 1), halo=pick(1, nx + 2), far=pick(0, nx + 3),
            to_halo=pick(nx + 2, 1), to_far=pick(nx + 3, 0), near_from=pick(2, nx + 1), far_from=pick(3, nx),
            both_from=pick(2, nx), both_to=pick(nx + 2, 0), both=pick(0, nx + 2))

    parity = lax.rem(gx, 2)
    order = (parity, 1 - parity)
    sides = [side_rows(side) for side in order]
    middle = pl.ds(8, nz - 16)

    def x_pieces(p):
        side, rows = order[p], sides[p]
        device = (lax.select(side == 0, along_x(-1)[0], along_x(1)[0]), gz)
        there = 1 - side
        plan = []
        for ks in (pl.ds(0, 8), pl.ds(nz - 8, 8)):
            plan.append((rows["both_from"], rows["both_to"], rows["both"], 2, ks, pl.ds(0, ny)))
        plan.append((rows["near_from"], rows["to_halo"], rows["halo"], 1, middle, pl.ds(0, ny)))
        for cols in tiles:
            plan.append((rows["far_from"], rows["to_far"], rows["far"], 1, middle, cols))
        out = []
        for n, (src, dst, here, deep, ks, cols) in enumerate(plan):
            send = remote(pad.at[:, pl.ds(src, deep), ks, cols], pad.at[:, pl.ds(dst, deep), ks, cols],
                          xs_sem.at[n, side], xr_sem.at[n, there], device)
            got = pad.at[:, pl.ds(here, deep), ks, cols]
            take = remote(got, got, xs_sem.at[n, side], xr_sem.at[n, side], device)
            out.append((send, take))
        return out

    pieces = [x_pieces(p) for p in range(2)]
    k_up = remote(pad.at[:, 2:nx + 2, nz - 2:nz], pad.at[:, 2:nx + 2, wide - 2:wide], ks_sem.at[0], kr_sem.at[0], along_z(1))
    k_down = remote(pad.at[:, 2:nx + 2, 0:2], pad.at[:, 2:nx + 2, nz:nz + 2], ks_sem.at[1], kr_sem.at[1], along_z(-1))

    for load in loads[:2]:
        load.wait()
    pl.semaphore_wait(barrier, 4)
    for pair in zip(*pieces):
        for send, _ in pair:
            send.start()
    loads[2].wait()
    k_up.start()
    k_down.start()

    know_x, know_z = doublings(gxn), doublings(gzn)
    direct = gxn * gzn <= DIRECT

    def learn_steps():
        last = max(len(know_x), len(know_z))
        for j in range(last + 1):
            if j > 0:
                for sem, steps in ((near_x, know_x), (near_z, know_z)):
                    if j <= len(steps):
                        pl.semaphore_wait(sem.at[j - 1], 2)
            for sem, steps, along in ((near_x, know_x, along_x), (near_z, know_z, along_z)):
                if j < len(steps):
                    signal(sem.at[j], along(steps[j]))
                    signal(sem.at[j], along(-steps[j]))
            if j < last:
                yield
        if direct and gzn > 1:
            for d in range(1, gzn):
                signal(near_all, along_z(d))
            yield
            pl.semaphore_wait(near_all, gzn - 1)

    steps = learn_steps()

    def learn():
        next(steps, None)

    learn()
    sums[...] = jnp.zeros_like(sums)
    gap_load.wait()
    span = gap_ref[:, 0:ny] + gap_ref[:, 1:ny + 1]
    at = lax.broadcasted_iota(jnp.int32, (1, ny), 1)
    width_sq = width_square(span)
    inverse = 2.0 / span
    coef_ref[0:1] = jnp.where(at == ny - 1, 0.0, inverse)
    coef_ref[1:2] = jnp.where(at == 0, 0.0, inverse)
    coef_ref[2:3] = width_sq * (1.0 / 256.0)
    coef_ref[3:4] = width_sq * width_sq * (1.0 / 256.0)
    coef_ref[4:5] = width_sq
    half_ahead, half_back = coef_ref[0:1, :], coef_ref[1:2, :]

    def filtered(f):
        twice = f + pltpu.roll(f, 1, 0)
        return twice + pltpu.roll(twice, wide - 1, 0)

    def lane_slope(f):
        return pltpu.roll(f, ny - 1, 1) * half_ahead - pltpu.roll(f, 1, 1) * half_back

    def smooth_tile(r, cols):
        for c in range(3):
            zvel[c, r, :, cols] = filtered(pad[c, r, :, cols])

    def smooth_row(r):
        for cols in tiles:
            smooth_tile(r, cols)

    def first_slope(r):
        for c in range(3):
            slope[c] = lane_slope(pad[c, r])

    def first_tile(r, cols, inside):
        u = [pad[c, r, :, cols] for c in range(3)]
        a = [pad[c, r + 1, :, cols] - pad[c, r - 1, :, cols] for c in range(3)]
        b = []
        for c in range(3):
            prev, nxt = pltpu.roll(u[c], 1, 0), pltpu.roll(u[c], wide - 1, 0)
            b.append(nxt - prev)
            if inside:
                zvel[c, r, :, cols] = (nxt + prev) + 2.0 * u[c]
        d = [slope[c, :, cols] for c in range(3)]
        strain = [a[0], d[1], b[2], d[0] + a[1], b[0] + a[2], b[1] + d[2]]
        square = [s * s for s in strain]
        size = jnp.sqrt(0.5 * (square[0] + square[1] + square[2]) + 0.25 * (square[3] + square[4] + square[5]))
        if inside:
            size_s[r - 2, :, cols] = size[:nz]
        for n in range(6):
            zstress[n, r, :, cols] = filtered(size * strain[n])[:nz]
        for n, (i, j) in enumerate(((0, 0), (1, 1), (2, 2), (0, 1), (0, 2), (1, 2))):
            zpair[n, r, :, cols] = filtered(u[i] * u[j])[:nz]

    def first(r, inside=True):
        first_slope(r)
        for cols in tiles:
            first_tile(r, cols, inside)

    def second_slope(r):
        for c in range(3):
            v = (zvel[c, r - 1] + zvel[c, r + 1]) + 2.0 * zvel[c, r]
            tslope[c] = v
            vslope[c] = lane_slope(v)

    def second_tile(r, cols):
        w = coef_ref[2:3, cols]
        w2 = coef_ref[3:4, cols]
        v_wide = [tslope[c, :, cols] for c in range(3)]
        v = [f[:nz] for f in v_wide]
        a = [(zvel[c, r + 2, 0:nz, cols] - zvel[c, r - 2, 0:nz, cols])
             + 2.0 * (zvel[c, r + 1, 0:nz, cols] - zvel[c, r - 1, 0:nz, cols]) for c in range(3)]
        b = [(pltpu.roll(f, wide - 1, 0) - pltpu.roll(f, 1, 0))[:nz] for f in v_wide]
        d = [vslope[c, 0:nz, cols] for c in range(3)]
        test = [a[0], d[1], b[2], d[0] + a[1], b[0] + a[2], b[1] + d[2]]
        square = [s * s for s in test]
        q = 0.25 * jnp.sqrt(0.5 * (square[0] + square[1] + square[2]) + 0.25 * (square[3] + square[4] + square[5]))
        lm, mm_diag, mm_off = 0.0, 0.0, 0.0
        for n, (i, j) in enumerate(((0, 0), (1, 1), (2, 2), (0, 1), (0, 2), (1, 2))):
            stress = (zstress[n, r - 1, :, cols] + zstress[n, r + 1, :, cols]) + 2.0 * zstress[n, r, :, cols]
            model = stress - q * test[n]
            pair = (zpair[n, r - 1, :, cols] + zpair[n, r + 1, :, cols]) + 2.0 * zpair[n, r, :, cols]
            lm = lm + (pair - v[i] * v[j] * 0.0625) * model
            if n < 3:
                mm_diag = mm_diag + model * model
            else:
                mm_off = mm_off + model * model
        lm = lm * w
        mm = (mm_diag + 0.5 * mm_off) * w2
        lm_s[r - 2, :, cols] = lm
        mm_s[r - 2, :, cols] = mm
        for n, f in enumerate((lm, mm)):
            sums[n, :, cols] += jnp.sum(f.reshape(nz // 8, 8, LANES), axis=0)

    def second(r):
        second_slope(r)
        for cols in tiles:
            second_tile(r, cols)

    def over(lo, hi, body):
        def step(r, carry):
            body(r)
            return carry
        lax.fori_loop(lo, hi, step, 0)

    k_up.wait_recv()
    k_down.wait_recv()
    learn()
    over(3, nx + 1, first)
    learn()
    smooth_row(2)
    smooth_row(nx + 1)

    def corner_copies(p):
        rows, out = pl.ds(sides[p]["both"], 2), []
        for n, (src, dst, device) in enumerate(((nz - 2, wide - 2, along_z(1)), (0, nz, along_z(-1)))):
            out.append(remote(pad.at[:, rows, pl.ds(src, 2)], pad.at[:, rows, pl.ds(dst, 2)], cs_sem.at[n, order[p]], cr_sem.at[n, order[p]], device))
        return out

    def relay(p):
        for _, take in pieces[p][:2]:
            take.wait_recv()
        for copy in corners[p]:
            copy.start()

    corners = [corner_copies(p) for p in range(2)]
    over(4, nx, second)
    learn()
    relay(0)
    relay(1)

    for _, take in pieces[0][2:]:
        take.wait_recv()
    for copy in corners[0]:
        copy.wait_recv()
    near = sides[0]

    def both(low, high, body):
        def step(n, carry):
            body(lax.select(n == 0, low, high))
            return carry
        lax.fori_loop(0, 2, step, 0)

    first(near["edge"])
    first(near["halo"], False)
    both(near["halo"], near["far"], smooth_row)
    both(near["inner"], near["edge"], second)
    learn()

    last = sides[1]
    pieces[1][2][1].wait_recv()
    for copy in corners[1]:
        copy.wait_recv()
    first(last["edge"])
    smooth_row(last["halo"])
    second(last["inner"])
    first_slope(last["halo"])
    second_slope(last["edge"])
    for cols, (_, take) in zip(tiles, pieces[1][3:]):
        take.wait_recv()
        first_tile(last["halo"], cols, False)
        smooth_tile(last["far"], cols)
        second_tile(last["edge"], cols)

    for _ in steps:
        pass
    total = jnp.sum(sums[...], axis=1)
    if direct:
        rounds = [(gx * gzn + gz, [(lax.rem(gx + dx, gxn), lax.rem(gz + dz, gzn))
                                   for dx in sorted(range(gxn), key=lambda d: -min(d, gxn - d))
                                   for dz in range(gzn) if dx or dz])]
    else:
        rounds = [(gz, [along_z(d) for d in range(1, gzn)]), (gx, [along_x(d) for d in range(1, gxn)])]
    sent = []
    for n, (slot, devices) in enumerate(rounds):
        acc, count = accs[n], len(devices)
        acc[slot] = total
        for device in devices:
            remote(acc.at[slot], acc.at[slot], as_sem.at[n], ar_sem.at[n], device).start()
        every = remote(acc.at[0:count], acc.at[0:count], as_sem.at[n], ar_sem.at[n], (gx, gz))
        every.wait_recv()
        sent.append(every)
        total = jnp.sum(acc[...], axis=0)
    coefficient = total[0:1] / cells / (total[1:2] / cells + 1e-06)
    out_coef_ref[0:1] = coefficient
    out_coef_ref[1:2] = coefficient * coef_ref[4:5]
    k_up.wait_send()
    k_down.wait_send()
    for p in range(2):
        for send, _ in pieces[p]:
            send.wait_send()
        for copy in corners[p]:
            copy.wait_send()
    for copy in sent:
        copy.wait_send()


def per_device(velocity, y_gap):
    gxn, gzn = lax.axis_size("gx"), lax.axis_size("gz")
    _, nx, nz, ny = velocity.shape
    cells = float(nx * gxn * nz * gzn)
    field = jax.ShapeDtypeStruct((nx, nz, ny), jnp.float32)
    f32 = jnp.float32
    wide = nz + RIM
    dma, flag = pltpu.SemaphoreType.DMA, pltpu.SemaphoreType.REGULAR
    members = (gxn * gzn,) if gxn * gzn <= DIRECT else (gzn, gxn)
    parts = 3 + ny // LANES
    gaps = y_gap.reshape(1, ny + 1)
    near = pl.BlockSpec(memory_space=pltpu.VMEM)
    far = pl.BlockSpec(memory_space=pl.ANY)
    held = pltpu.VMEM((nx, nz, ny), f32)
    size, lm, mm, coefficient = pl.pallas_call(
        functools.partial(kernel, gxn, gzn, cells),
        out_shape=(held, held, held, pltpu.VMEM((2, ny), f32)),
        in_specs=[far, far],
        out_specs=(near,) * 4,
        scratch_shapes=[
            pltpu.VMEM((3, nx + 4, wide, ny), f32),
            pltpu.VMEM((3, nx + 4, wide, ny), f32),
            pltpu.VMEM((6, nx + 4, nz, ny), f32),
            pltpu.VMEM((6, nx + 4, nz, ny), f32),
            pltpu.VMEM((3, wide, ny), f32),
            pltpu.VMEM((3, wide, ny), f32),
            pltpu.VMEM((3, wide, ny), f32),
            pltpu.VMEM((8, ny), f32),
            pltpu.VMEM((2, 8, ny), f32),
            tuple(pltpu.VMEM((n, 2, ny), f32) for n in members),
            pltpu.VMEM((1, ny + 1), f32), dma,
            dma((3,)), dma((parts, 2)), dma((parts, 2)), dma((2,)), dma((2,)), dma((2, 2)), dma((2, 2)),
            flag((max(len(doublings(gxn)), 1),)), flag((max(len(doublings(gzn)), 1),)), flag,
            dma((len(members),)), dma((len(members),)),
        ],
        compiler_params=pltpu.CompilerParams(
            collective_id=0, has_side_effects=True, vmem_limit_bytes=40 * 2**20),
    )(pltpu.with_memory_space_constraint(gaps, pltpu.HBM), pltpu.with_memory_space_constraint(velocity, pltpu.HBM))
    return pl.pallas_call(
        finish,
        out_shape=(field, field, field, jax.ShapeDtypeStruct((ny,), f32)),
        in_specs=[near] * 4,
        out_specs=(far, far, far, near),
        scratch_shapes=[pltpu.VMEM((nx, nz, ny), f32), dma((2 + (nx + 1) // 2,))],
        compiler_params=pltpu.CompilerParams(vmem_limit_bytes=8 * 2**20),
    )(size, lm, mm, coefficient)


def solution(mesh):
    placed = (P(None, "gx", "gz", None), P())
    return jax.shard_map(
        per_device,
        mesh=mesh,
        in_specs=placed,
        out_specs=(P("gx", "gz", None), P("gx", "gz", None), P("gx", "gz", None), P()),
        check_vma=False,
    )
```

```python
import functools

import jax
import jax.numpy as jnp
from jax import lax
from jax.experimental import pallas as pl
from jax.experimental.pallas import tpu as pltpu
from jax.sharding import PartitionSpec as P

MESH = pl.DeviceIdType.MESH
LANES = 128
RIM = 8
DIRECT = 64
EDGES, NEAR = (0, 1), (2, 3, 4)
PAIRS = ((0, 0), (1, 1), (2, 2), (0, 1), (0, 2), (1, 2))


def width_square(span):
    return jnp.exp(jnp.log(0.5 * span) * (2.0 / 3.0))


def finish(size_ref, lm_ref, mm_ref, coef_ref, eddy_out, lm_out, mm_out, coef_out, eddy_s, sem):
    nx, _, ny = size_ref.shape
    copies = [pltpu.make_async_copy(lm_ref, lm_out, sem.at[0]), pltpu.make_async_copy(mm_ref, mm_out, sem.at[1])]
    for copy in copies:
        copy.start()
    factor = coef_ref[1:2]
    for r in range(0, nx, 2):
        rows = pl.ds(r, 2)
        eddy_s[rows] = factor * size_ref[rows]
        copy = pltpu.make_async_copy(eddy_s.at[rows], eddy_out.at[rows], sem.at[2 + r // 2])
        copy.start()
        copies.append(copy)
    coef_out[...] = coef_ref[0:1].reshape(ny)
    for copy in copies:
        copy.wait()


def doublings(size):
    reach, steps = 1, []
    while reach < size // 2:
        steps.append(reach)
        reach *= 2
    return steps


def kernel(gxn, gzn, cells, gap_hbm, vel_ref, size_s, lm_s, mm_s, out_coef_ref,
           pad, zvel, zpair, zstress, slope, tslope, vslope, leon_ref, coef_ref, sums, accs,
           gap_ref, gap_sem, load_sem, xs_sem, xr_sem, ks_sem, kr_sem, cs_sem, cr_sem,
           near_x, near_z, near_all, as_sem, ar_sem):
    gx, gz = lax.axis_index("gx"), lax.axis_index("gz")
    nx, nz, ny = vel_ref.shape[1:]
    wide = nz + RIM
    tiles = [pl.ds(t, LANES) for t in range(0, ny, LANES)]

    def along_x(d):
        return (lax.rem(gx + d + gxn, gxn), gz)

    def along_z(d):
        return (gx, lax.rem(gz + d + gzn, gzn))

    def signal(sem, device):
        pl.semaphore_signal(sem, inc=1, device_id=device, device_id_type=MESH)

    def remote(src, dst, send, recv, device):
        return pltpu.make_async_remote_copy(
            src_ref=src, dst_ref=dst, send_sem=send, recv_sem=recv,
            device_id=device, device_id_type=MESH)

    barrier = pltpu.get_barrier_semaphore()
    for device in (along_x(1), along_x(-1), along_z(1), along_z(-1)):
        signal(barrier, device)
    loads = []
    for n, (lo, hi) in enumerate(((0, 2), (nx - 2, nx), (2, nx - 2))):
        loads.append(pltpu.make_async_copy(vel_ref.at[:, lo:hi], pad.at[:, lo + 2:hi + 2, 0:nz], load_sem.at[n]))
    for load in loads:
        load.start()
    gap_load = pltpu.make_async_copy(gap_hbm, gap_ref, gap_sem)
    gap_load.start()

    def side_rows(side):
        def pick(low, high):
            return lax.select(side == 0, low, high)
        return dict(
            inner=pick(3, nx), edge=pick(2, nx + 1), halo=pick(1, nx + 2), far=pick(0, nx + 3),
            to_halo=pick(nx + 2, 1), to_far=pick(nx + 3, 0), near_from=pick(2, nx + 1), far_from=pick(3, nx),
            both_from=pick(2, nx), both_to=pick(nx + 2, 0), both=pick(0, nx + 2))

    parity = lax.rem(gx, 2)
    order = (parity, 1 - parity)
    sides = [side_rows(side) for side in order]

    def x_pieces(p):
        side, rows = order[p], sides[p]
        device = (lax.select(side == 0, along_x(-1)[0], along_x(1)[0]), gz)
        there = 1 - side
        plan = []
        both = (2, rows["both_from"], rows["both_to"], rows["both"])
        near = (1, rows["near_from"], rows["to_halo"], rows["halo"])
        far = (1, rows["far_from"], rows["to_far"], rows["far"])
        for ks in (pl.ds(0, 2), pl.ds(nz - 2, 2)):
            plan.append((both, ks, pl.ds(0, ny)))
        inner = (pl.ds(2, 6), pl.ds(8, nz - 16), pl.ds(nz - 8, 6))
        for ks in inner:
            plan.append((near, ks, pl.ds(0, ny)))
        for cols in tiles:
            for ks in inner:
                plan.append((far, ks, cols))
        out = []
        for n, ((deep, src, dst, here), ks, cols) in enumerate(plan):
            give = remote(pad.at[:, pl.ds(src, deep), ks, cols], pad.at[:, pl.ds(dst, deep), ks, cols],
                          xs_sem.at[n, side], xr_sem.at[n, there], device)
            got = pad.at[:, pl.ds(here, deep), ks, cols]
            got = remote(got, got, xs_sem.at[n, side], xr_sem.at[n, side], device)
            out.append((give, got))
        return out

    pieces = [x_pieces(p) for p in range(2)]
    k_up = remote(pad.at[:, 2:nx + 2, nz - 2:nz], pad.at[:, 2:nx + 2, wide - 2:wide], ks_sem.at[0], kr_sem.at[0], along_z(1))
    k_down = remote(pad.at[:, 2:nx + 2, 0:2], pad.at[:, 2:nx + 2, nz:nz + 2], ks_sem.at[1], kr_sem.at[1], along_z(-1))

    def far(t):
        return tuple(range(5 + 3 * t, 8 + 3 * t))

    def send(*which):
        for n in which:
            for p in range(2):
                pieces[p][n][0].start()

    def take(*which):
        for n in which:
            for p in range(2):
                pieces[p][n][1].wait_recv()

    for load in loads[:2]:
        load.wait()
    pl.semaphore_wait(barrier, 4)
    send(*EDGES, *NEAR)
    loads[2].wait()
    k_up.start()
    k_down.start()

    know_x, know_z = doublings(gxn), doublings(gzn)
    direct = gxn * gzn <= DIRECT

    def learn_steps():
        last = max(len(know_x), len(know_z))
        for j in range(last + 1):
            if j > 0:
                for sem, steps in ((near_x, know_x), (near_z, know_z)):
                    if j <= len(steps):
                        pl.semaphore_wait(sem.at[j - 1], 2)
            for sem, steps, along in ((near_x, know_x, along_x), (near_z, know_z, along_z)):
                if j < len(steps):
                    signal(sem.at[j], along(steps[j]))
                    signal(sem.at[j], along(-steps[j]))
            if j < last:
                yield
        if direct and gzn > 1:
            for d in range(1, gzn):
                signal(near_all, along_z(d))
            yield
            pl.semaphore_wait(near_all, gzn - 1)

    steps = learn_steps()

    def learn():
        next(steps, None)

    learn()
    sums[...] = jnp.zeros_like(sums)
    gap_load.wait()
    span = gap_ref[:, 0:ny] + gap_ref[:, 1:ny + 1]
    at = lax.broadcasted_iota(jnp.int32, (1, ny), 1)
    width_sq = width_square(span)
    inverse = 2.0 / span
    coef_ref[0:1] = jnp.where(at == ny - 1, 0.0, inverse)
    coef_ref[1:2] = jnp.where(at == 0, 0.0, inverse)
    coef_ref[2:3] = width_sq * (1.0 / 256.0)
    coef_ref[3:4] = width_sq * width_sq * (1.0 / 256.0)
    coef_ref[4:5] = width_sq
    half_ahead, half_back = coef_ref[0:1, :], coef_ref[1:2, :]

    def filtered(f):
        twice = f + pltpu.roll(f, 1, 0)
        return twice + pltpu.roll(twice, wide - 1, 0)

    def lane_slope(f):
        return pltpu.roll(f, ny - 1, 1) * half_ahead - pltpu.roll(f, 1, 1) * half_back

    def smooth_tile(r, cols):
        for c in range(3):
            zvel[c, r, :, cols] = filtered(pad[c, r, :, cols])

    def smooth_row(r):
        for cols in tiles:
            smooth_tile(r, cols)

    def first_slope(r, n=2):
        for c in range(3):
            slope[n, c] = lane_slope(pad[c, r])

    def stress_tile(r, cols, inside, side=2):
        u = [pad[c, r, :, cols] for c in range(3)]
        a = [pad[c, r + 1, :, cols] - pad[c, r - 1, :, cols] for c in range(3)]
        b = []
        for c in range(3):
            prev, nxt = pltpu.roll(u[c], 1, 0), pltpu.roll(u[c], wide - 1, 0)
            b.append(nxt - prev)
            if inside:
                zvel[c, r, :, cols] = (nxt + prev) + 2.0 * u[c]
        d = [slope[side, c, :, cols] for c in range(3)]
        strain = [a[0], d[1], b[2], d[0] + a[1], b[0] + a[2], b[1] + d[2]]
        square = [s * s for s in strain]
        size = jnp.sqrt(0.5 * (square[0] + square[1] + square[2]) + 0.25 * (square[3] + square[4] + square[5]))
        if inside:
            size_s[r - 2, :, cols] = size[:nz]
        for n in range(6):
            zstress[n, r, :, cols] = filtered(size * strain[n])[:nz]

    def pair_tile(r, cols):
        u = [pad[c, r, :, cols] for c in range(3)]
        for n, (i, j) in enumerate(PAIRS):
            zpair[n, r, :, cols] = filtered(u[i] * u[j])[:nz]

    def first(r):
        first_slope(r)
        for cols in tiles:
            stress_tile(r, cols, True)
            pair_tile(r, cols)

    def second_slope(r, n=2):
        for c in range(3):
            v = (zvel[c, r - 1] + zvel[c, r + 1]) + 2.0 * zvel[c, r]
            tslope[n, c] = v
            vslope[n, c] = lane_slope(v)

    def leonard(r, cols, side=2):
        v = [tslope[side, c, 0:nz, cols] for c in range(3)]
        out = []
        for n, (i, j) in enumerate(PAIRS):
            pair = (zpair[n, r - 1, :, cols] + zpair[n, r + 1, :, cols]) + 2.0 * zpair[n, r, :, cols]
            out.append(pair - v[i] * v[j] * 0.0625)
        return out

    def second_tile(r, cols, side=2, leon=None):
        w = coef_ref[2:3, cols]
        w2 = coef_ref[3:4, cols]
        v_wide = [tslope[side, c, :, cols] for c in range(3)]
        a = [(zvel[c, r + 2, 0:nz, cols] - zvel[c, r - 2, 0:nz, cols])
             + 2.0 * (zvel[c, r + 1, 0:nz, cols] - zvel[c, r - 1, 0:nz, cols]) for c in range(3)]
        b = [(pltpu.roll(f, wide - 1, 0) - pltpu.roll(f, 1, 0))[:nz] for f in v_wide]
        d = [vslope[side, c, 0:nz, cols] for c in range(3)]
        test = [a[0], d[1], b[2], d[0] + a[1], b[0] + a[2], b[1] + d[2]]
        square = [s * s for s in test]
        q = 0.25 * jnp.sqrt(0.5 * (square[0] + square[1] + square[2]) + 0.25 * (square[3] + square[4] + square[5]))
        lm, mm_diag, mm_off = 0.0, 0.0, 0.0
        leon = leon or leonard(r, cols, side)
        for n in range(6):
            stress = (zstress[n, r - 1, :, cols] + zstress[n, r + 1, :, cols]) + 2.0 * zstress[n, r, :, cols]
            model = stress - q * test[n]
            lm = lm + leon[n] * model
            if n < 3:
                mm_diag = mm_diag + model * model
            else:
                mm_off = mm_off + model * model
        lm = lm * w
        mm = (mm_diag + 0.5 * mm_off) * w2
        lm_s[r - 2, :, cols] = lm
        mm_s[r - 2, :, cols] = mm
        for n, f in enumerate((lm, mm)):
            sums[n, :, cols] += jnp.sum(f.reshape(nz // 8, 8, LANES), axis=0)

    def second(r):
        second_slope(r)
        for cols in tiles:
            second_tile(r, cols)

    def over(lo, hi, body):
        def step(r, carry):
            body(r)
            return carry
        lax.fori_loop(lo, hi, step, 0)

    k_up.wait_recv()
    k_down.wait_recv()
    over(3, nx + 1, first)
    learn()
    take(*EDGES)
    relayed = []
    for p in range(2):
        rows = pl.ds(sides[p]["both"], 2)
        for n, (src, dst, device) in enumerate(((nz - 2, wide - 2, along_z(1)), (0, nz, along_z(-1)))):
            relayed.append(remote(pad.at[:, rows, pl.ds(src, 2)], pad.at[:, rows, pl.ds(dst, 2)], cs_sem.at[n, order[p]], cr_sem.at[n, order[p]], device))
    for copy in relayed:
        copy.start()
    send(*far(0))
    smooth_row(2)
    smooth_row(nx + 1)
    over(4, nx, second)
    send(*far(1))

    def both(body):
        for p in range(2):
            body(p, sides[p])

    take(*NEAR)
    send(*far(2))
    learn()
    for copy in relayed:
        copy.wait_recv()

    def ready(p, rows):
        first(rows["edge"])
        smooth_row(rows["halo"])
        second(rows["inner"])
        first_slope(rows["halo"], p)
        second_slope(rows["edge"], p)
        for cols in tiles:
            pair_tile(rows["halo"], cols)
            for n, f in enumerate(leonard(rows["edge"], cols, p)):
                leon_ref[p, n, :, cols] = f

    ready(0, sides[0])
    ready(1, sides[1])
    for _ in steps:
        pass
    here = gx * gzn + gz
    if direct:
        rounds = [(here, [(lax.rem(gx + dx, gxn), lax.rem(gz + dz, gzn))
                          for dx in sorted(range(gxn), key=lambda d: -min(d, gxn - d))
                          for dz in range(gzn) if dx or dz])]
    else:
        rounds = [(gz, [along_z(d) for d in range(1, gzn)]), (gx, [along_x(d) for d in range(1, gxn)])]

    def spread(n, t, value):
        slot, devices = rounds[n]
        acc = accs[n].at[t]
        acc[slot] = value
        for device in devices:
            remote(acc.at[slot], acc.at[slot], as_sem.at[n, t], ar_sem.at[n, t], device).start()

    def gathered(n, t):
        acc, count = accs[n].at[t], len(rounds[n][1])
        return remote(acc.at[0:count], acc.at[0:count], as_sem.at[n, t], ar_sem.at[n, t], (gx, gz))

    for t, cols in enumerate(tiles):
        take(*far(t))

        def finish_rows(p, rows):
            stress_tile(rows["halo"], cols, False, p)
            smooth_tile(rows["far"], cols)
            second_tile(rows["edge"], cols, p, [leon_ref[p, n, :, cols] for n in range(6)])

        both(finish_rows)
        spread(0, t, jnp.sum(sums[:, :, cols], axis=1))
    for n in range(1, len(rounds) + 1):
        for t, cols in enumerate(tiles):
            gathered(n - 1, t).wait_recv()
            total = jnp.sum(accs[n - 1][t], axis=0)
            if n < len(rounds):
                spread(n, t, total)
            else:
                coefficient = total[0:1] / cells / (total[1:2] / cells + 1e-06)
                out_coef_ref[0:1, cols] = coefficient
                out_coef_ref[1:2, cols] = coefficient * coef_ref[4:5, cols]
    sent = [gathered(n, t) for n in range(len(rounds)) for t in range(len(tiles))]
    k_up.wait_send()
    k_down.wait_send()
    for p in range(2):
        for copy, _ in pieces[p]:
            copy.wait_send()
    for copy in relayed + sent:
        copy.wait_send()


def per_device(velocity, y_gap):
    gxn, gzn = lax.axis_size("gx"), lax.axis_size("gz")
    _, nx, nz, ny = velocity.shape
    cells = float(nx * gxn * nz * gzn)
    field = jax.ShapeDtypeStruct((nx, nz, ny), jnp.float32)
    f32 = jnp.float32
    wide = nz + RIM
    dma, flag = pltpu.SemaphoreType.DMA, pltpu.SemaphoreType.REGULAR
    members = (gxn * gzn,) if gxn * gzn <= DIRECT else (gzn, gxn)
    parts = 5 + 3 * (ny // LANES)
    gaps = y_gap.reshape(1, ny + 1)
    near = pl.BlockSpec(memory_space=pltpu.VMEM)
    far = pl.BlockSpec(memory_space=pl.ANY)
    held = pltpu.VMEM((nx, nz, ny), f32)
    size, lm, mm, coefficient = pl.pallas_call(
        functools.partial(kernel, gxn, gzn, cells),
        out_shape=(held, held, held, pltpu.VMEM((2, ny), f32)),
        in_specs=[far, far],
        out_specs=(near,) * 4,
        scratch_shapes=[
            pltpu.VMEM((3, nx + 4, wide, ny), f32),
            pltpu.VMEM((3, nx + 4, wide, ny), f32),
            pltpu.VMEM((6, nx + 4, nz, ny), f32),
            pltpu.VMEM((6, nx + 4, nz, ny), f32),
            pltpu.VMEM((3, 3, wide, ny), f32),
            pltpu.VMEM((3, 3, wide, ny), f32),
            pltpu.VMEM((3, 3, wide, ny), f32),
            pltpu.VMEM((2, 6, nz, ny), f32),
            pltpu.VMEM((8, ny), f32),
            pltpu.VMEM((2, 8, ny), f32),
            tuple(pltpu.VMEM((ny // LANES, n, 2, LANES), f32) for n in members),
            pltpu.VMEM((1, ny + 1), f32), dma,
            dma((3,)), dma((parts, 2)), dma((parts, 2)), dma((2,)), dma((2,)), dma((2, 2)), dma((2, 2)),
            flag((max(len(doublings(gxn)), 1),)), flag((max(len(doublings(gzn)), 1),)), flag,
            dma((len(members), ny // LANES)), dma((len(members), ny // LANES)),
        ],
        compiler_params=pltpu.CompilerParams(
            collective_id=0, has_side_effects=True, vmem_limit_bytes=40 * 2**20),
    )(pltpu.with_memory_space_constraint(gaps, pltpu.HBM), pltpu.with_memory_space_constraint(velocity, pltpu.HBM))
    return pl.pallas_call(
        finish,
        out_shape=(field, field, field, jax.ShapeDtypeStruct((ny,), f32)),
        in_specs=[near] * 4,
        out_specs=(far, far, far, near),
        scratch_shapes=[pltpu.VMEM((nx, nz, ny), f32), dma((2 + (nx + 1) // 2,))],
        compiler_params=pltpu.CompilerParams(vmem_limit_bytes=8 * 2**20),
    )(size, lm, mm, coefficient)


def solution(mesh):
    placed = (P(None, "gx", "gz", None), P())
    return jax.shard_map(
        per_device,
        mesh=mesh,
        in_specs=placed,
        out_specs=(P("gx", "gz", None), P("gx", "gz", None), P("gx", "gz", None), P()),
        check_vma=False,
    )
```

```python
import functools

import jax
import jax.numpy as jnp
from jax import lax
from jax.experimental import pallas as pl
from jax.experimental.pallas import tpu as pltpu
from jax.sharding import PartitionSpec as P

MESH = pl.DeviceIdType.MESH
LANES = 128
RIM = 8
DIRECT = 64
EDGES, NEAR = (0, 1), (2, 3, 4)
PAIRS = ((0, 0), (1, 1), (2, 2), (0, 1), (0, 2), (1, 2))


def width_square(span):
    return jnp.exp(jnp.log(0.5 * span) * (2.0 / 3.0))


def finish(size_ref, lm_ref, mm_ref, coef_ref, eddy_out, lm_out, mm_out, coef_out, eddy_s, coef_s, sem):
    nx = size_ref.shape[0]
    copies = [pltpu.make_async_copy(lm_ref, lm_out, sem.at[0]), pltpu.make_async_copy(mm_ref, mm_out, sem.at[1])]
    coef_s[...] = coef_ref[0:1].reshape(coef_s.shape)
    copies.append(pltpu.make_async_copy(coef_s, coef_out, sem.at[2]))
    for copy in copies:
        copy.start()
    factor = coef_ref[1:2]
    for r in range(0, nx, 2):
        rows = pl.ds(r, 2)
        eddy_s[rows] = factor * size_ref[rows]
        pltpu.make_async_copy(eddy_s.at[rows], eddy_out.at[rows], sem.at[3]).start()
    copies.append(pltpu.make_async_copy(eddy_s, eddy_out, sem.at[3]))
    for copy in copies:
        copy.wait()


def doublings(size):
    reach, steps = 1, []
    while reach < size // 2:
        steps.append(reach)
        reach *= 2
    return steps


def kernel(gxn, gzn, cells, gap_hbm, vel_ref, size_s, lm_s, mm_s, out_coef_ref,
           pad, zvel, zpair, zstress, slope, tslope, vslope, leon_ref, coef_ref, sums, accs,
           gap_ref, gap_sem, load_sem, xs_sem, xr_sem, ks_sem, kr_sem, cs_sem, cr_sem,
           near_x, near_z, near_all, as_sem, ar_sem):
    gx, gz = lax.axis_index("gx"), lax.axis_index("gz")
    nx, nz, ny = vel_ref.shape[1:]
    wide = nz + RIM
    tiles = [pl.ds(t, LANES) for t in range(0, ny, LANES)]

    def along_x(d):
        return (lax.rem(gx + d + gxn, gxn), gz)

    def along_z(d):
        return (gx, lax.rem(gz + d + gzn, gzn))

    def signal(sem, device):
        pl.semaphore_signal(sem, inc=1, device_id=device, device_id_type=MESH)

    def remote(src, dst, send, recv, device):
        return pltpu.make_async_remote_copy(
            src_ref=src, dst_ref=dst, send_sem=send, recv_sem=recv,
            device_id=device, device_id_type=MESH)

    barrier = pltpu.get_barrier_semaphore()
    for device in (along_x(1), along_x(-1), along_z(1), along_z(-1)):
        signal(barrier, device)
    loads = []
    for n, (lo, hi) in enumerate(((0, 2), (nx - 2, nx), (2, nx - 2))):
        loads.append(pltpu.make_async_copy(vel_ref.at[:, lo:hi], pad.at[:, lo + 2:hi + 2, 0:nz], load_sem.at[n // 2]))
    for load in loads:
        load.start()
    gap_load = pltpu.make_async_copy(gap_hbm, gap_ref, gap_sem)
    gap_load.start()

    def side_rows(side):
        def pick(low, high):
            return lax.select(side == 0, low, high)
        return dict(
            inner=pick(3, nx), edge=pick(2, nx + 1), halo=pick(1, nx + 2), far=pick(0, nx + 3),
            to_halo=pick(nx + 2, 1), to_far=pick(nx + 3, 0), near_from=pick(2, nx + 1), far_from=pick(3, nx),
            both_from=pick(2, nx), both_to=pick(nx + 2, 0), both=pick(0, nx + 2))

    parity = lax.rem(gx, 2)
    order = (parity, 1 - parity)
    sides = [side_rows(side) for side in order]

    def group_of(n):
        return 0 if n in EDGES else 1 if n in NEAR else 2 + (n - 5) // 3

    def x_pieces(p):
        side, rows = order[p], sides[p]
        device = (lax.select(side == 0, along_x(-1)[0], along_x(1)[0]), gz)
        plan = []
        both = (2, rows["both_from"], rows["both_to"])
        near = (1, rows["near_from"], rows["to_halo"])
        far = (1, rows["far_from"], rows["to_far"])
        for ks in (pl.ds(0, 2), pl.ds(nz - 2, 2)):
            plan.append((*both, ks, pl.ds(0, ny)))
        inner = (pl.ds(2, 6), pl.ds(8, nz - 16), pl.ds(nz - 8, 6))
        for ks in inner:
            plan.append((*near, ks, pl.ds(0, ny)))
        for cols in tiles:
            for ks in inner:
                plan.append((*far, ks, cols))
        return [remote(pad.at[:, pl.ds(src, deep), ks, cols], pad.at[:, pl.ds(dst, deep), ks, cols],
                       xs_sem, xr_sem.at[group_of(n)], device)
                for n, (deep, src, dst, ks, cols) in enumerate(plan)]

    pieces = [x_pieces(p) for p in range(2)]
    k_up = remote(pad.at[:, 2:nx + 2, nz - 2:nz], pad.at[:, 2:nx + 2, wide - 2:wide], ks_sem, kr_sem, along_z(1))
    k_down = remote(pad.at[:, 2:nx + 2, 0:2], pad.at[:, 2:nx + 2, nz:nz + 2], ks_sem, kr_sem, along_z(-1))

    def far(t):
        return tuple(range(5 + 3 * t, 8 + 3 * t))

    def wait_for(columns, sem, cols=pl.ds(0, ny)):
        ref = pad.at[:, 0:columns // 8, 0:8, cols]
        remote(ref, ref, sem, sem, (gx, gz)).wait_recv()

    def send(*which):
        for n in which:
            for p in range(2):
                pieces[p][n].start()

    pltpu.make_async_copy(vel_ref.at[:, 0:4], pad.at[:, 0:4, 0:nz], load_sem.at[0]).wait()
    pl.semaphore_wait(barrier, 4)
    send(*EDGES, *NEAR)
    loads[2].wait()
    k_up.start()
    k_down.start()

    know_x, know_z = doublings(gxn), doublings(gzn)
    direct = gxn * gzn <= DIRECT

    def learn_steps():
        last = max(len(know_x), len(know_z))
        for j in range(last + 1):
            if j > 0:
                for sem, steps in ((near_x, know_x), (near_z, know_z)):
                    if j <= len(steps):
                        pl.semaphore_wait(sem.at[j - 1], 2)
            for sem, steps, along in ((near_x, know_x, along_x), (near_z, know_z, along_z)):
                if j < len(steps):
                    signal(sem.at[j], along(steps[j]))
                    signal(sem.at[j], along(-steps[j]))
            if j < last:
                yield
        if direct and gzn > 1:
            for d in range(1, gzn):
                signal(near_all, along_z(d))
            yield
            pl.semaphore_wait(near_all, gzn - 1)

    steps = learn_steps()

    def learn():
        next(steps, None)

    learn()
    sums[...] = jnp.zeros_like(sums)
    gap_load.wait()
    span = gap_ref[:, 0:ny] + gap_ref[:, 1:ny + 1]
    at = lax.broadcasted_iota(jnp.int32, (1, ny), 1)
    width_sq = width_square(span)
    inverse = 2.0 / span
    coef_ref[0:1] = jnp.where(at == ny - 1, 0.0, inverse)
    coef_ref[1:2] = jnp.where(at == 0, 0.0, inverse)
    coef_ref[2:3] = width_sq * (1.0 / 256.0)
    coef_ref[3:4] = width_sq * width_sq * (1.0 / 256.0)
    coef_ref[4:5] = width_sq
    half_ahead, half_back = coef_ref[0:1, :], coef_ref[1:2, :]

    def filtered(f):
        twice = f + pltpu.roll(f, 1, 0)
        return twice + pltpu.roll(twice, wide - 1, 0)

    def lane_slope(f):
        return pltpu.roll(f, ny - 1, 1) * half_ahead - pltpu.roll(f, 1, 1) * half_back

    def smooth_tile(r, cols):
        for c in range(3):
            zvel[c, r, :, cols] = filtered(pad[c, r, :, cols])

    def smooth_row(r):
        for cols in tiles:
            smooth_tile(r, cols)

    def first_slope(r, n=2):
        for c in range(3):
            slope[n, c] = lane_slope(pad[c, r])

    def stress_tile(r, cols, inside, side=2):
        u = [pad[c, r, :, cols] for c in range(3)]
        a = [pad[c, r + 1, :, cols] - pad[c, r - 1, :, cols] for c in range(3)]
        b = []
        for c in range(3):
            prev, nxt = pltpu.roll(u[c], 1, 0), pltpu.roll(u[c], wide - 1, 0)
            b.append(nxt - prev)
            if inside:
                zvel[c, r, :, cols] = (nxt + prev) + 2.0 * u[c]
        d = [slope[side, c, :, cols] for c in range(3)]
        strain = [a[0], d[1], b[2], d[0] + a[1], b[0] + a[2], b[1] + d[2]]
        square = [s * s for s in strain]
        size = jnp.sqrt(0.5 * (square[0] + square[1] + square[2]) + 0.25 * (square[3] + square[4] + square[5]))
        if inside:
            size_s[r - 2, :, cols] = size[:nz]
        for n in range(6):
            zstress[n, r, :, cols] = filtered(size * strain[n])[:nz]

    def pair_tile(r, cols):
        u = [pad[c, r, :, cols] for c in range(3)]
        for n, (i, j) in enumerate(PAIRS):
            zpair[n, r, :, cols] = filtered(u[i] * u[j])[:nz]

    def first(r):
        first_slope(r)
        for cols in tiles:
            stress_tile(r, cols, True)
            pair_tile(r, cols)

    def second_slope(r, n=2):
        for c in range(3):
            v = (zvel[c, r - 1] + zvel[c, r + 1]) + 2.0 * zvel[c, r]
            tslope[n, c] = v
            vslope[n, c] = lane_slope(v)

    def leonard(r, cols, side=2):
        v = [tslope[side, c, 0:nz, cols] for c in range(3)]
        out = []
        for n, (i, j) in enumerate(PAIRS):
            pair = (zpair[n, r - 1, :, cols] + zpair[n, r + 1, :, cols]) + 2.0 * zpair[n, r, :, cols]
            out.append(pair - v[i] * v[j] * 0.0625)
        return out

    def second_tile(r, cols, side=2, leon=None):
        w = coef_ref[2:3, cols]
        w2 = coef_ref[3:4, cols]
        v_wide = [tslope[side, c, :, cols] for c in range(3)]
        a = [(zvel[c, r + 2, 0:nz, cols] - zvel[c, r - 2, 0:nz, cols])
             + 2.0 * (zvel[c, r + 1, 0:nz, cols] - zvel[c, r - 1, 0:nz, cols]) for c in range(3)]
        b = [(pltpu.roll(f, wide - 1, 0) - pltpu.roll(f, 1, 0))[:nz] for f in v_wide]
        d = [vslope[side, c, 0:nz, cols] for c in range(3)]
        test = [a[0], d[1], b[2], d[0] + a[1], b[0] + a[2], b[1] + d[2]]
        square = [s * s for s in test]
        q = 0.25 * jnp.sqrt(0.5 * (square[0] + square[1] + square[2]) + 0.25 * (square[3] + square[4] + square[5]))
        lm, mm_diag, mm_off = 0.0, 0.0, 0.0
        leon = leon or leonard(r, cols, side)
        for n in range(6):
            stress = (zstress[n, r - 1, :, cols] + zstress[n, r + 1, :, cols]) + 2.0 * zstress[n, r, :, cols]
            model = stress - q * test[n]
            lm = lm + leon[n] * model
            if n < 3:
                mm_diag = mm_diag + model * model
            else:
                mm_off = mm_off + model * model
        lm = lm * w
        mm = (mm_diag + 0.5 * mm_off) * w2
        lm_s[r - 2, :, cols] = lm
        mm_s[r - 2, :, cols] = mm
        for n, f in enumerate((lm, mm)):
            sums[n, :, cols] += jnp.sum(f.reshape(nz // 8, 8, LANES), axis=0)

    def second(r):
        second_slope(r)
        for cols in tiles:
            second_tile(r, cols)

    def over(lo, hi, body):
        def step(r, carry):
            body(r)
            return carry
        lax.fori_loop(lo, hi, step, 0)

    wait_for(4 * nx, kr_sem)
    over(3, nx + 1, first)
    learn()
    smooth_row(2)
    smooth_row(nx + 1)
    over(4, nx, second)
    send(*far(0))
    send(*far(1))
    wait_for(16, xr_sem.at[0])
    relayed = []
    for p in range(2):
        rows = pl.ds(sides[p]["both"], 2)
        for n, (src, dst, device) in enumerate(((nz - 2, wide - 2, along_z(1)), (0, nz, along_z(-1)))):
            relayed.append(remote(pad.at[:, rows, pl.ds(src, 2)], pad.at[:, rows, pl.ds(dst, 2)], cs_sem, cr_sem, device))
    for copy in relayed:
        copy.start()

    def both(body):
        for p in range(2):
            body(p, sides[p])

    wait_for(2 * (nz - 4), xr_sem.at[1])
    send(*far(2))
    learn()
    wait_for(16, cr_sem)

    def ready(p, rows):
        first(rows["edge"])
        smooth_row(rows["halo"])
        second(rows["inner"])
        first_slope(rows["halo"], p)
        second_slope(rows["edge"], p)
        for cols in tiles:
            pair_tile(rows["halo"], cols)
            for n, f in enumerate(leonard(rows["edge"], cols, p)):
                leon_ref[p, n, :, cols] = f

    ready(0, sides[0])
    ready(1, sides[1])
    for _ in steps:
        pass
    here = gx * gzn + gz
    if direct:
        rounds = [(here, [(lax.rem(gx + dx, gxn), lax.rem(gz + dz, gzn))
                          for dx in sorted(range(gxn), key=lambda d: -min(d, gxn - d))
                          for dz in range(gzn) if dx or dz])]
    else:
        rounds = [(gz, [along_z(d) for d in range(1, gzn)]), (gx, [along_x(d) for d in range(1, gxn)])]

    def spread(n, t, value):
        slot, devices = rounds[n]
        acc = accs[n].at[t]
        acc[slot] = value
        for device in devices:
            remote(acc.at[slot], acc.at[slot], as_sem.at[n], ar_sem.at[n, t], device).start()

    def gathered(n, t):
        acc, count = accs[n].at[t], len(rounds[n][1])
        return remote(acc.at[0:count], acc.at[0:count], as_sem.at[n], ar_sem.at[n, t], (gx, gz))

    for t, cols in enumerate(tiles):
        wait_for(2 * (nz - 4), xr_sem.at[2 + t], tiles[0])

        def finish_rows(p, rows):
            stress_tile(rows["halo"], cols, False, p)
            smooth_tile(rows["far"], cols)
            second_tile(rows["edge"], cols, p, [leon_ref[p, n, :, cols] for n in range(6)])

        both(finish_rows)
        spread(0, t, jnp.sum(sums[:, :, cols], axis=1))
    for n in range(1, len(rounds) + 1):
        for t, cols in enumerate(tiles):
            gathered(n - 1, t).wait_recv()
            total = jnp.sum(accs[n - 1][t], axis=0)
            if n < len(rounds):
                spread(n, t, total)
            else:
                coefficient = total[0:1] / cells / (total[1:2] / cells + 1e-06)
                out_coef_ref[0:1, cols] = coefficient
                out_coef_ref[1:2, cols] = coefficient * coef_ref[4:5, cols]
    wait_for(4 * nx, ks_sem)
    block = pad.at[:, 0:4, 0:nz]
    remote(block, block, xs_sem, xs_sem, (gx, gz)).wait_send()
    wait_for(16, cs_sem)
    for n, (_, devices) in enumerate(rounds):
        acc = accs[n].at[:, 0:len(devices)]
        remote(acc, acc, as_sem.at[n], as_sem.at[n], (gx, gz)).wait_send()


def per_device(velocity, y_gap):
    gxn, gzn = lax.axis_size("gx"), lax.axis_size("gz")
    _, nx, nz, ny = velocity.shape
    cells = float(nx * gxn * nz * gzn)
    field = jax.ShapeDtypeStruct((nx, nz, ny), jnp.float32)
    f32 = jnp.float32
    wide = nz + RIM
    dma, flag = pltpu.SemaphoreType.DMA, pltpu.SemaphoreType.REGULAR
    members = (gxn * gzn,) if gxn * gzn <= DIRECT else (gzn, gxn)
    gaps = y_gap.reshape(1, ny + 1)
    near = pl.BlockSpec(memory_space=pltpu.VMEM)
    far = pl.BlockSpec(memory_space=pl.ANY)
    held = pltpu.VMEM((nx, nz, ny), f32)
    size, lm, mm, coefficient = pl.pallas_call(
        functools.partial(kernel, gxn, gzn, cells),
        out_shape=(held, held, held, pltpu.VMEM((2, ny), f32)),
        in_specs=[far, far],
        out_specs=(near,) * 4,
        scratch_shapes=[
            pltpu.VMEM((3, nx + 4, wide, ny), f32),
            pltpu.VMEM((3, nx + 4, wide, ny), f32),
            pltpu.VMEM((6, nx + 4, nz, ny), f32),
            pltpu.VMEM((6, nx + 4, nz, ny), f32),
            pltpu.VMEM((3, 3, wide, ny), f32),
            pltpu.VMEM((3, 3, wide, ny), f32),
            pltpu.VMEM((3, 3, wide, ny), f32),
            pltpu.VMEM((2, 6, nz, ny), f32),
            pltpu.VMEM((8, ny), f32),
            pltpu.VMEM((2, 8, ny), f32),
            tuple(pltpu.VMEM((ny // LANES, n, 2, LANES), f32) for n in members),
            pltpu.VMEM((1, ny + 1), f32), dma,
            dma((2,)), dma, dma((2 + ny // LANES,)), dma, dma, dma, dma,
            flag((max(len(doublings(gxn)), 1),)), flag((max(len(doublings(gzn)), 1),)), flag,
            dma((len(members),)), dma((len(members), ny // LANES)),
        ],
        compiler_params=pltpu.CompilerParams(
            collective_id=0, has_side_effects=True, vmem_limit_bytes=40 * 2**20),
    )(pltpu.with_memory_space_constraint(gaps, pltpu.HBM), pltpu.with_memory_space_constraint(velocity, pltpu.HBM))
    return pl.pallas_call(
        finish,
        out_shape=(field, field, field, jax.ShapeDtypeStruct((ny,), f32)),
        in_specs=[near] * 4,
        out_specs=(far,) * 4,
        scratch_shapes=[pltpu.VMEM((nx, nz, ny), f32), pltpu.VMEM((ny,), f32), dma((4,))],
        compiler_params=pltpu.CompilerParams(vmem_limit_bytes=8 * 2**20),
    )(size, lm, mm, coefficient)


def solution(mesh):
    placed = (P(None, "gx", "gz", None), P())
    return jax.shard_map(
        per_device,
        mesh=mesh,
        in_specs=placed,
        out_specs=(P("gx", "gz", None), P("gx", "gz", None), P("gx", "gz", None), P()),
        check_vma=False,
    )
```

```python
import functools

import jax
import jax.numpy as jnp
from jax import lax
from jax.experimental import pallas as pl
from jax.experimental.pallas import tpu as pltpu
from jax.sharding import PartitionSpec as P

MESH = pl.DeviceIdType.MESH
LANES = 128
RIM = 8
DIRECT = 64
EDGES, NEAR = (0, 1), (2, 3, 4)
PAIRS = ((0, 0), (1, 1), (2, 2), (0, 1), (0, 2), (1, 2))


def width_square(span):
    return jnp.exp(jnp.log(0.5 * span) * (2.0 / 3.0))


def finish(size_ref, lm_ref, mm_ref, coef_ref, eddy_out, lm_out, mm_out, coef_out, eddy_s, coef_s, sem):
    nx = size_ref.shape[0]
    copies = [pltpu.make_async_copy(lm_ref, lm_out, sem.at[0]), pltpu.make_async_copy(mm_ref, mm_out, sem.at[1])]
    coef_s[...] = coef_ref[0:1].reshape(coef_s.shape)
    copies.append(pltpu.make_async_copy(coef_s, coef_out, sem.at[2]))
    for copy in copies:
        copy.start()
    factor = coef_ref[1:2]
    for r in range(0, nx, 2):
        rows = pl.ds(r, 2)
        eddy_s[rows] = factor * size_ref[rows]
        pltpu.make_async_copy(eddy_s.at[rows], eddy_out.at[rows], sem.at[3]).start()
    copies.append(pltpu.make_async_copy(eddy_s, eddy_out, sem.at[3]))
    for copy in copies:
        copy.wait()


def doublings(size):
    reach, steps = 1, []
    while reach < size // 2:
        steps.append(reach)
        reach *= 2
    return steps


def kernel(gxn, gzn, cells, gap_hbm, vel_ref, size_s, lm_s, mm_s, out_coef_ref,
           pad, zvel, zpair, zstress, slope, tslope, vslope, leon_ref, coef_ref, sums, accs,
           gap_ref, gap_sem, load_sem, xs_sem, xr_sem, ks_sem, kr_sem, cs_sem, cr_sem,
           near_x, near_z, near_all, as_sem, ar_sem):
    gx, gz = lax.axis_index("gx"), lax.axis_index("gz")
    nx, nz, ny = vel_ref.shape[1:]
    wide = nz + RIM
    tiles = [pl.ds(t, LANES) for t in range(0, ny, LANES)]

    def along_x(d):
        return (lax.rem(gx + d + gxn, gxn), gz)

    def along_z(d):
        return (gx, lax.rem(gz + d + gzn, gzn))

    def signal(sem, device):
        pl.semaphore_signal(sem, inc=1, device_id=device, device_id_type=MESH)

    def remote(src, dst, send, recv, device):
        return pltpu.make_async_remote_copy(
            src_ref=src, dst_ref=dst, send_sem=send, recv_sem=recv,
            device_id=device, device_id_type=MESH)

    barrier = pltpu.get_barrier_semaphore()
    for device in (along_x(1), along_x(-1), along_z(1), along_z(-1)):
        signal(barrier, device)
    loads = []
    for n, (lo, hi) in enumerate(((0, 2), (nx - 2, nx), (2, nx - 2))):
        loads.append(pltpu.make_async_copy(vel_ref.at[:, lo:hi], pad.at[:, lo + 2:hi + 2, 0:nz], load_sem.at[n // 2]))
    for load in loads:
        load.start()
    gap_load = pltpu.make_async_copy(gap_hbm, gap_ref, gap_sem)
    gap_load.start()

    def side_rows(side):
        def pick(low, high):
            return lax.select(side == 0, low, high)
        return dict(
            inner=pick(3, nx), edge=pick(2, nx + 1), halo=pick(1, nx + 2), far=pick(0, nx + 3),
            to_halo=pick(nx + 2, 1), to_far=pick(nx + 3, 0), near_from=pick(2, nx + 1), far_from=pick(3, nx),
            both_from=pick(2, nx), both_to=pick(nx + 2, 0), both=pick(0, nx + 2))

    parity = lax.rem(gx, 2)
    order = (parity, 1 - parity)
    sides = [side_rows(side) for side in order]

    def group_of(n):
        return 0 if n in EDGES else 1 if n in NEAR else 2 + (n - 5) // 3

    def x_pieces(p):
        side, rows = order[p], sides[p]
        device = (lax.select(side == 0, along_x(-1)[0], along_x(1)[0]), gz)
        plan = []
        both = (2, rows["both_from"], rows["both_to"])
        near = (1, rows["near_from"], rows["to_halo"])
        far = (1, rows["far_from"], rows["to_far"])
        for ks in (pl.ds(0, 2), pl.ds(nz - 2, 2)):
            plan.append((*both, ks, pl.ds(0, ny)))
        inner = (pl.ds(2, 6), pl.ds(8, nz - 16), pl.ds(nz - 8, 6))
        for ks in inner:
            plan.append((*near, ks, pl.ds(0, ny)))
        for cols in tiles:
            for ks in inner:
                plan.append((*far, ks, cols))
        return [remote(pad.at[:, pl.ds(src, deep), ks, cols], pad.at[:, pl.ds(dst, deep), ks, cols],
                       xs_sem, xr_sem.at[group_of(n)], device)
                for n, (deep, src, dst, ks, cols) in enumerate(plan)]

    pieces = [x_pieces(p) for p in range(2)]
    k_up = remote(pad.at[:, 2:nx + 2, nz - 2:nz], pad.at[:, 2:nx + 2, wide - 2:wide], ks_sem, kr_sem, along_z(1))
    k_down = remote(pad.at[:, 2:nx + 2, 0:2], pad.at[:, 2:nx + 2, nz:nz + 2], ks_sem, kr_sem, along_z(-1))

    def far(t):
        return tuple(range(5 + 3 * t, 8 + 3 * t))

    def wait_for(columns, sem, cols=pl.ds(0, ny)):
        ref = pad.at[:, 0:columns // 8, 0:8, cols]
        remote(ref, ref, sem, sem, (gx, gz)).wait_recv()

    def send(*which):
        for n in which:
            for p in range(2):
                pieces[p][n].start()

    pltpu.make_async_copy(vel_ref.at[:, 0:4], pad.at[:, 0:4, 0:nz], load_sem.at[0]).wait()
    pl.semaphore_wait(barrier, 4)
    send(*EDGES, *NEAR)
    loads[2].wait()
    k_up.start()
    k_down.start()

    know_x, know_z = doublings(gxn), doublings(gzn)
    direct = gxn * gzn <= DIRECT

    def learn_steps():
        last = max(len(know_x), len(know_z))
        for j in range(last + 1):
            if j > 0:
                for sem, steps in ((near_x, know_x), (near_z, know_z)):
                    if j <= len(steps):
                        pl.semaphore_wait(sem.at[j - 1], 2)
            for sem, steps, along in ((near_x, know_x, along_x), (near_z, know_z, along_z)):
                if j < len(steps):
                    signal(sem.at[j], along(steps[j]))
                    signal(sem.at[j], along(-steps[j]))
            if j < last:
                yield
        if direct and gzn > 1:
            for d in range(1, gzn):
                signal(near_all, along_z(d))
            yield
            pl.semaphore_wait(near_all, gzn - 1)

    steps = learn_steps()

    def learn():
        next(steps, None)

    learn()
    sums[...] = jnp.zeros_like(sums)
    gap_load.wait()
    span = gap_ref[:, 0:ny] + gap_ref[:, 1:ny + 1]
    at = lax.broadcasted_iota(jnp.int32, (1, ny), 1)
    width_sq = width_square(span)
    inverse = 2.0 / span
    coef_ref[0:1] = jnp.where(at == ny - 1, 0.0, inverse)
    coef_ref[1:2] = jnp.where(at == 0, 0.0, inverse)
    coef_ref[2:3] = width_sq * (1.0 / 256.0)
    coef_ref[3:4] = width_sq * width_sq * (1.0 / 256.0)
    coef_ref[4:5] = width_sq
    half_ahead, half_back = coef_ref[0:1, :], coef_ref[1:2, :]

    def filtered(f):
        twice = f + pltpu.roll(f, 1, 0)
        return twice + pltpu.roll(twice, wide - 1, 0)

    def lane_slope(f):
        return pltpu.roll(f, ny - 1, 1) * half_ahead - pltpu.roll(f, 1, 1) * half_back

    def smooth_tile(r, cols):
        for c in range(3):
            zvel[c, r, :, cols] = filtered(pad[c, r, :, cols])

    def smooth_row(r):
        for cols in tiles:
            smooth_tile(r, cols)

    def first_slope(r, n=2):
        for c in range(3):
            slope[n, c] = lane_slope(pad[c, r])

    def stress_tile(r, cols, inside, side=2):
        u = [pad[c, r, :, cols] for c in range(3)]
        a = [pad[c, r + 1, :, cols] - pad[c, r - 1, :, cols] for c in range(3)]
        b = []
        for c in range(3):
            prev, nxt = pltpu.roll(u[c], 1, 0), pltpu.roll(u[c], wide - 1, 0)
            b.append(nxt - prev)
            if inside:
                zvel[c, r, :, cols] = (nxt + prev) + 2.0 * u[c]
        d = [slope[side, c, :, cols] for c in range(3)]
        strain = [a[0], d[1], b[2], d[0] + a[1], b[0] + a[2], b[1] + d[2]]
        square = [s * s for s in strain]
        size = jnp.sqrt(0.5 * (square[0] + square[1] + square[2]) + 0.25 * (square[3] + square[4] + square[5]))
        if inside:
            size_s[r - 2, :, cols] = size[:nz]
        for n in range(6):
            zstress[n, r, :, cols] = filtered(size * strain[n])[:nz]

    def pair_tile(r, cols):
        u = [pad[c, r, :, cols] for c in range(3)]
        for n, (i, j) in enumerate(PAIRS):
            zpair[n, r, :, cols] = filtered(u[i] * u[j])[:nz]

    def first(r):
        first_slope(r)
        for cols in tiles:
            stress_tile(r, cols, True)
            pair_tile(r, cols)

    def second_slope(r, n=2):
        for c in range(3):
            v = (zvel[c, r - 1] + zvel[c, r + 1]) + 2.0 * zvel[c, r]
            tslope[n, c] = v
            vslope[n, c] = lane_slope(v)

    def leonard(r, cols, side=2):
        v = [tslope[side, c, 0:nz, cols] for c in range(3)]
        out = []
        for n, (i, j) in enumerate(PAIRS):
            pair = (zpair[n, r - 1, :, cols] + zpair[n, r + 1, :, cols]) + 2.0 * zpair[n, r, :, cols]
            out.append(pair - v[i] * v[j] * 0.0625)
        return out

    def second_tile(r, cols, side=2, leon=None):
        w = coef_ref[2:3, cols]
        w2 = coef_ref[3:4, cols]
        v_wide = [tslope[side, c, :, cols] for c in range(3)]
        a = [(zvel[c, r + 2, 0:nz, cols] - zvel[c, r - 2, 0:nz, cols])
             + 2.0 * (zvel[c, r + 1, 0:nz, cols] - zvel[c, r - 1, 0:nz, cols]) for c in range(3)]
        b = [(pltpu.roll(f, wide - 1, 0) - pltpu.roll(f, 1, 0))[:nz] for f in v_wide]
        d = [vslope[side, c, 0:nz, cols] for c in range(3)]
        test = [a[0], d[1], b[2], d[0] + a[1], b[0] + a[2], b[1] + d[2]]
        square = [s * s for s in test]
        q = 0.25 * jnp.sqrt(0.5 * (square[0] + square[1] + square[2]) + 0.25 * (square[3] + square[4] + square[5]))
        lm, mm_diag, mm_off = 0.0, 0.0, 0.0
        leon = leon or leonard(r, cols, side)
        for n in range(6):
            stress = (zstress[n, r - 1, :, cols] + zstress[n, r + 1, :, cols]) + 2.0 * zstress[n, r, :, cols]
            model = stress - q * test[n]
            lm = lm + leon[n] * model
            if n < 3:
                mm_diag = mm_diag + model * model
            else:
                mm_off = mm_off + model * model
        lm = lm * w
        mm = (mm_diag + 0.5 * mm_off) * w2
        lm_s[r - 2, :, cols] = lm
        mm_s[r - 2, :, cols] = mm
        for n, f in enumerate((lm, mm)):
            sums[n, :, cols] += jnp.sum(f.reshape(nz // 8, 8, LANES), axis=0)

    def second(r):
        second_slope(r)
        for cols in tiles:
            second_tile(r, cols)

    def over(lo, hi, body):
        def step(r, carry):
            body(r)
            return carry
        lax.fori_loop(lo, hi, step, 0)

    wait_for(4 * nx, kr_sem)
    over(3, nx + 1, first)
    learn()
    smooth_row(2)
    smooth_row(nx + 1)
    over(4, nx, second)
    send(*far(0))
    send(*far(1))
    wait_for(16, xr_sem.at[0])
    relayed = []
    for p in range(2):
        rows = pl.ds(sides[p]["both"], 2)
        for n, (src, dst, device) in enumerate(((nz - 2, wide - 2, along_z(1)), (0, nz, along_z(-1)))):
            relayed.append(remote(pad.at[:, rows, pl.ds(src, 2)], pad.at[:, rows, pl.ds(dst, 2)], cs_sem, cr_sem, device))
    for copy in relayed:
        copy.start()

    def both(body):
        for p in range(2):
            body(p, sides[p])

    wait_for(2 * (nz - 4), xr_sem.at[1])
    send(*far(2))
    learn()
    wait_for(16, cr_sem)

    def ready(p, rows):
        first(rows["edge"])
        smooth_row(rows["halo"])
        second(rows["inner"])
        first_slope(rows["halo"], p)
        second_slope(rows["edge"], p)
        for cols in tiles:
            pair_tile(rows["halo"], cols)
            for n, f in enumerate(leonard(rows["edge"], cols, p)):
                leon_ref[p, n, :, cols] = f

    ready(0, sides[0])
    ready(1, sides[1])
    for _ in steps:
        pass
    here = gx * gzn + gz
    if direct:
        rounds = [(here, [(ox, oz) for ox in range(gxn) for oz in range(gzn)], gxn * gzn - 1)]
    else:
        rounds = [(gz, [(gx, oz) for oz in range(gzn)], gzn - 1), (gx, [(ox, gz) for ox in range(gxn)], gxn - 1)]

    def spread(n, t, value):
        slot, devices, _ = rounds[n]
        acc = accs[n].at[t]
        acc[slot] = value
        for device in devices:
            @pl.when((device[0] != gx) | (device[1] != gz))
            def _():
                remote(acc.at[slot], acc.at[slot], as_sem.at[n], ar_sem.at[n, t], device).start()

    def gathered(n, t):
        acc, count = accs[n].at[t], rounds[n][2]
        return remote(acc.at[0:count], acc.at[0:count], as_sem.at[n], ar_sem.at[n, t], (gx, gz))

    for t, cols in enumerate(tiles):
        wait_for(2 * (nz - 4), xr_sem.at[2 + t], tiles[0])

        def finish_rows(p, rows):
            stress_tile(rows["halo"], cols, False, p)
            smooth_tile(rows["far"], cols)
            second_tile(rows["edge"], cols, p, [leon_ref[p, n, :, cols] for n in range(6)])

        both(finish_rows)
        spread(0, t, jnp.sum(sums[:, :, cols], axis=1))
    for n in range(1, len(rounds) + 1):
        for t, cols in enumerate(tiles):
            gathered(n - 1, t).wait_recv()
            total = jnp.sum(accs[n - 1][t], axis=0)
            if n < len(rounds):
                spread(n, t, total)
            else:
                coefficient = total[0:1] / cells / (total[1:2] / cells + 1e-06)
                out_coef_ref[0:1, cols] = coefficient
                out_coef_ref[1:2, cols] = coefficient * coef_ref[4:5, cols]
    wait_for(4 * nx, ks_sem)
    block = pad.at[:, 0:4, 0:nz]
    remote(block, block, xs_sem, xs_sem, (gx, gz)).wait_send()
    wait_for(16, cs_sem)
    for n, (_, _, count) in enumerate(rounds):
        acc = accs[n].at[:, 0:count]
        remote(acc, acc, as_sem.at[n], as_sem.at[n], (gx, gz)).wait_send()


def per_device(velocity, y_gap):
    gxn, gzn = lax.axis_size("gx"), lax.axis_size("gz")
    _, nx, nz, ny = velocity.shape
    cells = float(nx * gxn * nz * gzn)
    field = jax.ShapeDtypeStruct((nx, nz, ny), jnp.float32)
    f32 = jnp.float32
    wide = nz + RIM
    dma, flag = pltpu.SemaphoreType.DMA, pltpu.SemaphoreType.REGULAR
    members = (gxn * gzn,) if gxn * gzn <= DIRECT else (gzn, gxn)
    gaps = y_gap.reshape(1, ny + 1)
    near = pl.BlockSpec(memory_space=pltpu.VMEM)
    far = pl.BlockSpec(memory_space=pl.ANY)
    held = pltpu.VMEM((nx, nz, ny), f32)
    size, lm, mm, coefficient = pl.pallas_call(
        functools.partial(kernel, gxn, gzn, cells),
        out_shape=(held, held, held, pltpu.VMEM((2, ny), f32)),
        in_specs=[far, far],
        out_specs=(near,) * 4,
        scratch_shapes=[
            pltpu.VMEM((3, nx + 4, wide, ny), f32),
            pltpu.VMEM((3, nx + 4, wide, ny), f32),
            pltpu.VMEM((6, nx + 4, nz, ny), f32),
            pltpu.VMEM((6, nx + 4, nz, ny), f32),
            pltpu.VMEM((3, 3, wide, ny), f32),
            pltpu.VMEM((3, 3, wide, ny), f32),
            pltpu.VMEM((3, 3, wide, ny), f32),
            pltpu.VMEM((2, 6, nz, ny), f32),
            pltpu.VMEM((8, ny), f32),
            pltpu.VMEM((2, 8, ny), f32),
            tuple(pltpu.VMEM((ny // LANES, n, 2, LANES), f32) for n in members),
            pltpu.VMEM((1, ny + 1), f32), dma,
            dma((2,)), dma, dma((2 + ny // LANES,)), dma, dma, dma, dma,
            flag((max(len(doublings(gxn)), 1),)), flag((max(len(doublings(gzn)), 1),)), flag,
            dma((len(members),)), dma((len(members), ny // LANES)),
        ],
        compiler_params=pltpu.CompilerParams(
            collective_id=0, has_side_effects=True, vmem_limit_bytes=40 * 2**20),
    )(pltpu.with_memory_space_constraint(gaps, pltpu.HBM), pltpu.with_memory_space_constraint(velocity, pltpu.HBM))
    return pl.pallas_call(
        finish,
        out_shape=(field, field, field, jax.ShapeDtypeStruct((ny,), f32)),
        in_specs=[near] * 4,
        out_specs=(far,) * 4,
        scratch_shapes=[pltpu.VMEM((nx, nz, ny), f32), pltpu.VMEM((ny,), f32), dma((4,))],
        compiler_params=pltpu.CompilerParams(vmem_limit_bytes=8 * 2**20),
    )(size, lm, mm, coefficient)


def solution(mesh):
    placed = (P(None, "gx", "gz", None), P())
    return jax.shard_map(
        per_device,
        mesh=mesh,
        in_specs=placed,
        out_specs=(P("gx", "gz", None), P("gx", "gz", None), P("gx", "gz", None), P()),
        check_vma=False,
    )
```

```python
import functools

import jax
import jax.numpy as jnp
from jax import lax
from jax.experimental import pallas as pl
from jax.experimental.pallas import tpu as pltpu
from jax.sharding import PartitionSpec as P

MESH = pl.DeviceIdType.MESH
LANES = 128
RIM = 8
DIRECT = 64
EDGES, NEAR = (0, 1), (2, 3, 4)
PAIRS = ((0, 0), (1, 1), (2, 2), (0, 1), (0, 2), (1, 2))


def width_square(span):
    return jnp.exp(jnp.log(0.5 * span) * (2.0 / 3.0))


def finish(size_ref, lm_ref, mm_ref, coef_ref, eddy_out, lm_out, mm_out, coef_out, eddy_s, coef_s, sem):
    nx = size_ref.shape[0]
    copies = [pltpu.make_async_copy(lm_ref, lm_out, sem.at[0]), pltpu.make_async_copy(mm_ref, mm_out, sem.at[1])]
    coef_s[...] = coef_ref[0:1].reshape(coef_s.shape)
    copies.append(pltpu.make_async_copy(coef_s, coef_out, sem.at[2]))
    for copy in copies:
        copy.start()
    factor = coef_ref[1:2]
    for r in range(0, nx, 2):
        rows = pl.ds(r, 2)
        eddy_s[rows] = factor * size_ref[rows]
        pltpu.make_async_copy(eddy_s.at[rows], eddy_out.at[rows], sem.at[3]).start()
    copies.append(pltpu.make_async_copy(eddy_s, eddy_out, sem.at[3]))
    for copy in copies:
        copy.wait()


def doublings(size):
    reach, steps = 1, []
    while reach < size // 2:
        steps.append(reach)
        reach *= 2
    return steps


def kernel(gxn, gzn, cells, gap_hbm, vel_ref, size_s, lm_s, mm_s, out_coef_ref,
           pad, zvel, zpair, zstress, slope, tslope, vslope, strain_ref, test_ref, rest_ref, leon_ref, coef_ref, sums, accs,
           gap_ref, gap_sem, load_sem, xs_sem, xr_sem, ks_sem, kr_sem, cs_sem, cr_sem,
           near_x, near_z, near_all, as_sem, ar_sem):
    gx, gz = lax.axis_index("gx"), lax.axis_index("gz")
    nx, nz, ny = vel_ref.shape[1:]
    wide = nz + RIM
    tiles = [pl.ds(t, LANES) for t in range(0, ny, LANES)]

    def along_x(d):
        return (lax.rem(gx + d + gxn, gxn), gz)

    def along_z(d):
        return (gx, lax.rem(gz + d + gzn, gzn))

    def signal(sem, device):
        pl.semaphore_signal(sem, inc=1, device_id=device, device_id_type=MESH)

    def remote(src, dst, send, recv, device):
        return pltpu.make_async_remote_copy(
            src_ref=src, dst_ref=dst, send_sem=send, recv_sem=recv,
            device_id=device, device_id_type=MESH)

    barrier = pltpu.get_barrier_semaphore()
    for device in (along_x(1), along_x(-1), along_z(1), along_z(-1)):
        signal(barrier, device)
    loads = []
    for n, (lo, hi) in enumerate(((0, 2), (nx - 2, nx), (2, nx - 2))):
        loads.append(pltpu.make_async_copy(vel_ref.at[:, lo:hi], pad.at[:, lo + 2:hi + 2, 0:nz], load_sem.at[n // 2]))
    for load in loads:
        load.start()
    gap_load = pltpu.make_async_copy(gap_hbm, gap_ref, gap_sem)
    gap_load.start()

    def side_rows(side):
        def pick(low, high):
            return lax.select(side == 0, low, high)
        return dict(
            other=pick(4, nx - 1), inner=pick(3, nx), edge=pick(2, nx + 1), halo=pick(1, nx + 2), far=pick(0, nx + 3),
            to_halo=pick(nx + 2, 1), to_far=pick(nx + 3, 0), near_from=pick(2, nx + 1), far_from=pick(3, nx),
            both_from=pick(2, nx), both_to=pick(nx + 2, 0), both=pick(0, nx + 2))

    parity = lax.rem(gx, 2)
    order = (parity, 1 - parity)
    sides = [side_rows(side) for side in order]
    signs = [lax.select(side == 0, 1.0, -1.0) for side in order]

    def group_of(n):
        return 0 if n in EDGES else 1 if n in NEAR else 2 + (n - 5) // 3

    def x_pieces(p):
        side, rows = order[p], sides[p]
        device = (lax.select(side == 0, along_x(-1)[0], along_x(1)[0]), gz)
        plan = []
        both = (2, rows["both_from"], rows["both_to"])
        near = (1, rows["near_from"], rows["to_halo"])
        far = (1, rows["far_from"], rows["to_far"])
        for ks in (pl.ds(0, 2), pl.ds(nz - 2, 2)):
            plan.append((*both, ks, pl.ds(0, ny)))
        inner = (pl.ds(2, 6), pl.ds(8, nz - 16), pl.ds(nz - 8, 6))
        for ks in inner:
            plan.append((*near, ks, pl.ds(0, ny)))
        for cols in tiles:
            for ks in inner:
                plan.append((*far, ks, cols))
        return [remote(pad.at[:, pl.ds(src, deep), ks, cols], pad.at[:, pl.ds(dst, deep), ks, cols],
                       xs_sem, xr_sem.at[group_of(n)], device)
                for n, (deep, src, dst, ks, cols) in enumerate(plan)]

    pieces = [x_pieces(p) for p in range(2)]
    k_up = remote(pad.at[:, 2:nx + 2, nz - 2:nz], pad.at[:, 2:nx + 2, wide - 2:wide], ks_sem, kr_sem, along_z(1))
    k_down = remote(pad.at[:, 2:nx + 2, 0:2], pad.at[:, 2:nx + 2, nz:nz + 2], ks_sem, kr_sem, along_z(-1))

    def far(t):
        return tuple(range(5 + 3 * t, 8 + 3 * t))

    def wait_for(columns, sem, cols=pl.ds(0, ny)):
        ref = pad.at[:, 0:columns // 8, 0:8, cols]
        remote(ref, ref, sem, sem, (gx, gz)).wait_recv()

    def send(*which):
        for n in which:
            for p in range(2):
                pieces[p][n].start()

    pltpu.make_async_copy(vel_ref.at[:, 0:4], pad.at[:, 0:4, 0:nz], load_sem.at[0]).wait()
    pl.semaphore_wait(barrier, 4)
    send(*EDGES, *NEAR)
    loads[2].wait()
    k_up.start()
    k_down.start()

    know_x, know_z = doublings(gxn), doublings(gzn)
    direct = gxn * gzn <= DIRECT

    def learn_steps():
        last = max(len(know_x), len(know_z))
        for j in range(last + 1):
            if j > 0:
                for sem, steps in ((near_x, know_x), (near_z, know_z)):
                    if j <= len(steps):
                        pl.semaphore_wait(sem.at[j - 1], 2)
            for sem, steps, along in ((near_x, know_x, along_x), (near_z, know_z, along_z)):
                if j < len(steps):
                    signal(sem.at[j], along(steps[j]))
                    signal(sem.at[j], along(-steps[j]))
            if j < last:
                yield
        if direct and gzn > 1:
            for d in range(1, gzn):
                signal(near_all, along_z(d))
            yield
            pl.semaphore_wait(near_all, gzn - 1)

    steps = learn_steps()

    def learn():
        next(steps, None)

    learn()
    sums[...] = jnp.zeros_like(sums)
    gap_load.wait()
    span = gap_ref[:, 0:ny] + gap_ref[:, 1:ny + 1]
    at = lax.broadcasted_iota(jnp.int32, (1, ny), 1)
    width_sq = width_square(span)
    inverse = 2.0 / span
    coef_ref[0:1] = jnp.where(at == ny - 1, 0.0, inverse)
    coef_ref[1:2] = jnp.where(at == 0, 0.0, inverse)
    coef_ref[2:3] = width_sq * (1.0 / 256.0)
    coef_ref[3:4] = width_sq * width_sq * (1.0 / 256.0)
    coef_ref[4:5] = width_sq
    half_ahead, half_back = coef_ref[0:1, :], coef_ref[1:2, :]

    def filtered(f):
        twice = f + pltpu.roll(f, 1, 0)
        return twice + pltpu.roll(twice, wide - 1, 0)

    def lane_slope(f):
        return pltpu.roll(f, ny - 1, 1) * half_ahead - pltpu.roll(f, 1, 1) * half_back

    def smooth_tile(r, cols):
        for c in range(3):
            zvel[c, r, :, cols] = filtered(pad[c, r, :, cols])

    def smooth_row(r):
        for cols in tiles:
            smooth_tile(r, cols)

    def first_slope(r):
        for c in range(3):
            slope[c] = lane_slope(pad[c, r])

    def strain_size(f):
        square = [s * s for s in f]
        return jnp.sqrt(0.5 * (square[0] + square[1] + square[2]) + 0.25 * (square[3] + square[4] + square[5]))

    def stress_tile(r, cols):
        u = [pad[c, r, :, cols] for c in range(3)]
        a = [pad[c, r + 1, :, cols] - pad[c, r - 1, :, cols] for c in range(3)]
        b = []
        for c in range(3):
            prev, nxt = pltpu.roll(u[c], 1, 0), pltpu.roll(u[c], wide - 1, 0)
            b.append(nxt - prev)
            zvel[c, r, :, cols] = (nxt + prev) + 2.0 * u[c]
        d = [slope[c, :, cols] for c in range(3)]
        strain = [a[0], d[1], b[2], d[0] + a[1], b[0] + a[2], b[1] + d[2]]
        size = strain_size(strain)
        size_s[r - 2, :, cols] = size[:nz]
        for n in range(6):
            zstress[n, r, :, cols] = filtered(size * strain[n])[:nz]

    def pair_tile(r, cols):
        u = [pad[c, r, :, cols] for c in range(3)]
        for n, (i, j) in enumerate(PAIRS):
            zpair[n, r, :, cols] = filtered(u[i] * u[j])[:nz]

    def first(r):
        first_slope(r)
        for cols in tiles:
            stress_tile(r, cols)
            pair_tile(r, cols)

    def second_slope(r):
        for c in range(3):
            v = (zvel[c, r - 1] + zvel[c, r + 1]) + 2.0 * zvel[c, r]
            tslope[c] = v
            vslope[c] = lane_slope(v)

    def leonard(r, cols):
        v = [tslope[c, 0:nz, cols] for c in range(3)]
        out = []
        for n, (i, j) in enumerate(PAIRS):
            pair = (zpair[n, r - 1, :, cols] + zpair[n, r + 1, :, cols]) + 2.0 * zpair[n, r, :, cols]
            out.append(pair - v[i] * v[j] * 0.0625)
        return out

    def contract(r, cols, test, stress, leon):
        w = coef_ref[2:3, cols]
        w2 = coef_ref[3:4, cols]
        q = 0.25 * strain_size(test)
        lm, mm_diag, mm_off = 0.0, 0.0, 0.0
        for n in range(6):
            model = stress[n] - q * test[n]
            lm = lm + leon[n] * model
            if n < 3:
                mm_diag = mm_diag + model * model
            else:
                mm_off = mm_off + model * model
        lm = lm * w
        mm = (mm_diag + 0.5 * mm_off) * w2
        lm_s[r - 2, :, cols] = lm
        mm_s[r - 2, :, cols] = mm
        for n, f in enumerate((lm, mm)):
            sums[n, :, cols] += jnp.sum(f.reshape(nz // 8, 8, LANES), axis=0)

    def second_tile(r, cols):
        v_wide = [tslope[c, :, cols] for c in range(3)]
        a = [(zvel[c, r + 2, 0:nz, cols] - zvel[c, r - 2, 0:nz, cols])
             + 2.0 * (zvel[c, r + 1, 0:nz, cols] - zvel[c, r - 1, 0:nz, cols]) for c in range(3)]
        b = [(pltpu.roll(f, wide - 1, 0) - pltpu.roll(f, 1, 0))[:nz] for f in v_wide]
        d = [vslope[c, 0:nz, cols] for c in range(3)]
        test = [a[0], d[1], b[2], d[0] + a[1], b[0] + a[2], b[1] + d[2]]
        stress = [(zstress[n, r - 1, :, cols] + zstress[n, r + 1, :, cols]) + 2.0 * zstress[n, r, :, cols] for n in range(6)]
        contract(r, cols, test, stress, leonard(r, cols))

    def second(r):
        second_slope(r)
        for cols in tiles:
            second_tile(r, cols)

    def over(lo, hi, body):
        def step(r, carry):
            body(r)
            return carry
        lax.fori_loop(lo, hi, step, 0)

    wait_for(4 * nx, kr_sem)
    over(3, nx + 1, first)
    learn()
    smooth_row(2)
    smooth_row(nx + 1)
    over(4, nx, second)
    send(*far(0))
    send(*far(1))
    wait_for(16, xr_sem.at[0])
    relayed = []
    for p in range(2):
        rows = pl.ds(sides[p]["both"], 2)
        for n, (src, dst, device) in enumerate(((nz - 2, wide - 2, along_z(1)), (0, nz, along_z(-1)))):
            relayed.append(remote(pad.at[:, rows, pl.ds(src, 2)], pad.at[:, rows, pl.ds(dst, 2)], cs_sem, cr_sem, device))
    for copy in relayed:
        copy.start()

    def both(body):
        for p in range(2):
            body(p, sides[p])

    wait_for(2 * (nz - 4), xr_sem.at[1])
    send(*far(2))
    learn()
    wait_for(16, cr_sem)

    def ready(p, rows):
        halo, edge = rows["halo"], rows["edge"]
        first(edge)
        smooth_row(halo)
        second(rows["inner"])
        first_slope(halo)
        second_slope(edge)
        for cols in tiles:
            pair_tile(halo, cols)
            u = [pad[c, halo, :, cols] for c in range(3)]
            b = [pltpu.roll(f, wide - 1, 0) - pltpu.roll(f, 1, 0) for f in u]
            d = [slope[c, :, cols] for c in range(3)]
            for n, f in enumerate((d[1], b[2], d[0], b[0], b[1] + d[2])):
                strain_ref[p, n, :, cols] = f
            v = [tslope[c, :, cols] for c in range(3)]
            b = [(pltpu.roll(f, wide - 1, 0) - pltpu.roll(f, 1, 0))[:nz] for f in v]
            a = [signs[p] * zvel[c, rows["other"], 0:nz, cols] + 2.0 * (zvel[c, edge + 1, 0:nz, cols] - zvel[c, edge - 1, 0:nz, cols])
                 for c in range(3)]
            d = [vslope[c, 0:nz, cols] for c in range(3)]
            leon = leonard(edge, cols)
            for n, f in enumerate((a[0], d[1], b[2], d[0] + a[1], b[0] + a[2], b[1] + d[2])):
                test_ref[p, n, :, cols] = f
                leon_ref[p, n, :, cols] = leon[n]
                rest_ref[p, n, :, cols] = zstress[n, rows["inner"], :, cols] + 2.0 * zstress[n, edge, :, cols]

    ready(0, sides[0])
    ready(1, sides[1])
    for _ in steps:
        pass
    here = gx * gzn + gz
    if direct:
        rounds = [(here, [(ox, oz) for ox in range(gxn) for oz in range(gzn)], gxn * gzn - 1)]
    else:
        rounds = [(gz, [(gx, oz) for oz in range(gzn)], gzn - 1), (gx, [(ox, gz) for ox in range(gxn)], gxn - 1)]

    def spread(n, t, value):
        slot, devices, _ = rounds[n]
        acc = accs[n].at[t]
        acc[slot] = value
        for device in devices:
            @pl.when((device[0] != gx) | (device[1] != gz))
            def _():
                remote(acc.at[slot], acc.at[slot], as_sem.at[n], ar_sem.at[n, t], device).start()

    def gathered(n, t):
        acc, count = accs[n].at[t], rounds[n][2]
        return remote(acc.at[0:count], acc.at[0:count], as_sem.at[n], ar_sem.at[n, t], (gx, gz))

    for t, cols in enumerate(tiles):
        wait_for(2 * (nz - 4), xr_sem.at[2 + t], tiles[0])

        def finish_rows(p, rows):
            u = [pad[c, rows["far"], :, cols] for c in range(3)]
            a = [signs[p] * (pad[c, rows["edge"], :, cols] - u[c]) for c in range(3)]
            part = [strain_ref[p, n, :, cols] for n in range(5)]
            strain = [a[0], part[0], part[1], part[2] + a[1], part[3] + a[2], part[4]]
            size = strain_size(strain)
            part = [test_ref[p, n, :, cols] for n in range(6)]
            a = [signs[p] * filtered(f)[:nz] for f in u]
            test = [part[0] - a[0], part[1], part[2], part[3] - a[1], part[4] - a[2], part[5]]
            stress = [rest_ref[p, n, :, cols] + filtered(size * strain[n])[:nz] for n in range(6)]
            contract(rows["edge"], cols, test, stress, [leon_ref[p, n, :, cols] for n in range(6)])

        both(finish_rows)
        spread(0, t, jnp.sum(sums[:, :, cols], axis=1))
    for n in range(1, len(rounds) + 1):
        for t, cols in enumerate(tiles):
            gathered(n - 1, t).wait_recv()
            total = jnp.sum(accs[n - 1][t], axis=0)
            if n < len(rounds):
                spread(n, t, total)
            else:
                coefficient = total[0:1] / cells / (total[1:2] / cells + 1e-06)
                out_coef_ref[0:1, cols] = coefficient
                out_coef_ref[1:2, cols] = coefficient * coef_ref[4:5, cols]
    wait_for(4 * nx, ks_sem)
    block = pad.at[:, 0:4, 0:nz]
    remote(block, block, xs_sem, xs_sem, (gx, gz)).wait_send()
    wait_for(16, cs_sem)
    for n, (_, _, count) in enumerate(rounds):
        acc = accs[n].at[:, 0:count]
        remote(acc, acc, as_sem.at[n], as_sem.at[n], (gx, gz)).wait_send()


def per_device(velocity, y_gap):
    gxn, gzn = lax.axis_size("gx"), lax.axis_size("gz")
    _, nx, nz, ny = velocity.shape
    cells = float(nx * gxn * nz * gzn)
    field = jax.ShapeDtypeStruct((nx, nz, ny), jnp.float32)
    f32 = jnp.float32
    wide = nz + RIM
    dma, flag = pltpu.SemaphoreType.DMA, pltpu.SemaphoreType.REGULAR
    members = (gxn * gzn,) if gxn * gzn <= DIRECT else (gzn, gxn)
    gaps = y_gap.reshape(1, ny + 1)
    near = pl.BlockSpec(memory_space=pltpu.VMEM)
    far = pl.BlockSpec(memory_space=pl.ANY)
    held = pltpu.VMEM((nx, nz, ny), f32)
    size, lm, mm, coefficient = pl.pallas_call(
        functools.partial(kernel, gxn, gzn, cells),
        out_shape=(held, held, held, pltpu.VMEM((2, ny), f32)),
        in_specs=[far, far],
        out_specs=(near,) * 4,
        scratch_shapes=[
            pltpu.VMEM((3, nx + 4, wide, ny), f32),
            pltpu.VMEM((3, nx + 4, wide, ny), f32),
            pltpu.VMEM((6, nx + 4, nz, ny), f32),
            pltpu.VMEM((6, nx + 4, nz, ny), f32),
            pltpu.VMEM((3, wide, ny), f32),
            pltpu.VMEM((3, wide, ny), f32),
            pltpu.VMEM((3, wide, ny), f32),
            pltpu.VMEM((2, 5, wide, ny), f32),
            pltpu.VMEM((2, 6, nz, ny), f32),
            pltpu.VMEM((2, 6, nz, ny), f32),
            pltpu.VMEM((2, 6, nz, ny), f32),
            pltpu.VMEM((8, ny), f32),
            pltpu.VMEM((2, 8, ny), f32),
            tuple(pltpu.VMEM((ny // LANES, n, 2, LANES), f32) for n in members),
            pltpu.VMEM((1, ny + 1), f32), dma,
            dma((2,)), dma, dma((2 + ny // LANES,)), dma, dma, dma, dma,
            flag((max(len(doublings(gxn)), 1),)), flag((max(len(doublings(gzn)), 1),)), flag,
            dma((len(members),)), dma((len(members), ny // LANES)),
        ],
        compiler_params=pltpu.CompilerParams(
            collective_id=0, has_side_effects=True, vmem_limit_bytes=40 * 2**20),
    )(pltpu.with_memory_space_constraint(gaps, pltpu.HBM), pltpu.with_memory_space_constraint(velocity, pltpu.HBM))
    return pl.pallas_call(
        finish,
        out_shape=(field, field, field, jax.ShapeDtypeStruct((ny,), f32)),
        in_specs=[near] * 4,
        out_specs=(far,) * 4,
        scratch_shapes=[pltpu.VMEM((nx, nz, ny), f32), pltpu.VMEM((ny,), f32), dma((4,))],
        compiler_params=pltpu.CompilerParams(vmem_limit_bytes=8 * 2**20),
    )(size, lm, mm, coefficient)


def solution(mesh):
    placed = (P(None, "gx", "gz", None), P())
    return jax.shard_map(
        per_device,
        mesh=mesh,
        in_specs=placed,
        out_specs=(P("gx", "gz", None), P("gx", "gz", None), P("gx", "gz", None), P()),
        check_vma=False,
    )
```

```python
import functools

import jax
import jax.numpy as jnp
from jax import lax
from jax.experimental import pallas as pl
from jax.experimental.pallas import tpu as pltpu
from jax.sharding import PartitionSpec as P

MESH = pl.DeviceIdType.MESH
LANES = 128
RIM = 8
DIRECT = 64
EDGES, NEAR = (0, 1), (2, 3, 4)
PAIRS = ((0, 0), (1, 1), (2, 2), (0, 1), (0, 2), (1, 2))


def width_square(span):
    return jnp.exp(jnp.log(0.5 * span) * (2.0 / 3.0))


def finish(size_ref, lm_ref, mm_ref, coef_ref, eddy_out, lm_out, mm_out, coef_out, eddy_s, coef_s, sem):
    nx = size_ref.shape[0]
    copies = [pltpu.make_async_copy(lm_ref, lm_out, sem.at[0]), pltpu.make_async_copy(mm_ref, mm_out, sem.at[1])]
    coef_s[...] = coef_ref[0:1].reshape(coef_s.shape)
    copies.append(pltpu.make_async_copy(coef_s, coef_out, sem.at[2]))
    for copy in copies:
        copy.start()
    factor = coef_ref[1:2]
    for r in range(0, nx, 2):
        rows = pl.ds(r, 2)
        eddy_s[rows] = factor * size_ref[rows]
        pltpu.make_async_copy(eddy_s.at[rows], eddy_out.at[rows], sem.at[3]).start()
    copies.append(pltpu.make_async_copy(eddy_s, eddy_out, sem.at[3]))
    for copy in copies:
        copy.wait()


def doublings(size):
    reach, steps = 1, []
    while reach < size // 2:
        steps.append(reach)
        reach *= 2
    return steps


def kernel(gxn, gzn, cells, gap_hbm, vel_ref, size_s, lm_s, mm_s, out_coef_ref,
           pad, zvel, zpair, zstress, slope, tslope, vslope, strain_ref, test_ref, rest_ref, leon_ref, coef_ref, sums, accs, via_ref, count_ref,
           gap_ref, gap_sem, load_sem, xs_sem, xr_sem, ks_sem, kr_sem, cs_sem, cr_sem,
           near_x, near_z, near_all, wrap_sem, via_sem, as_sem, ar_sem):
    gx, gz = lax.axis_index("gx"), lax.axis_index("gz")
    nx, nz, ny = vel_ref.shape[1:]
    wide = nz + RIM
    tiles = [pl.ds(t, LANES) for t in range(0, ny, LANES)]

    def along_x(d):
        return (lax.rem(gx + d + gxn, gxn), gz)

    def along_z(d):
        return (gx, lax.rem(gz + d + gzn, gzn))

    def signal(sem, device):
        pl.semaphore_signal(sem, inc=1, device_id=device, device_id_type=MESH)

    def remote(src, dst, send, recv, device):
        return pltpu.make_async_remote_copy(
            src_ref=src, dst_ref=dst, send_sem=send, recv_sem=recv,
            device_id=device, device_id_type=MESH)

    barrier = pltpu.get_barrier_semaphore()
    for device in (along_x(-1), along_z(1), along_z(-1)):
        signal(barrier, device)
    ahead, behind = gx < gxn - 1, gx > 0

    @pl.when(ahead)
    def _():
        signal(barrier, along_x(1))

    loads = []
    for n, (lo, hi) in enumerate(((0, 2), (nx - 2, nx), (2, nx - 2))):
        loads.append(pltpu.make_async_copy(vel_ref.at[:, lo:hi], pad.at[:, lo + 2:hi + 2, 0:nz], load_sem.at[n // 2]))
    for load in loads:
        load.start()
    gap_load = pltpu.make_async_copy(gap_hbm, gap_ref, gap_sem)
    gap_load.start()

    def side_rows(side):
        def pick(low, high):
            return lax.select(side == 0, low, high)
        return dict(
            other=pick(4, nx - 1), inner=pick(3, nx), edge=pick(2, nx + 1), halo=pick(1, nx + 2), far=pick(0, nx + 3),
            to_halo=pick(nx + 2, 1), to_far=pick(nx + 3, 0), near_from=pick(2, nx + 1), far_from=pick(3, nx),
            both_from=pick(2, nx), both_to=pick(nx + 2, 0), both=pick(0, nx + 2))

    parity = lax.rem(gx, 2)
    order = (parity, 1 - parity)
    sides = [side_rows(side) for side in order]
    signs = [lax.select(side == 0, 1.0, -1.0) for side in order]

    def group_of(n):
        return 0 if n in EDGES else 1 if n in NEAR else 2 + (n - 5) // 3

    inner = (pl.ds(2, 6), pl.ds(8, nz - 16), pl.ds(nz - 8, 6))

    def x_pieces(p):
        side, rows = order[p], sides[p]
        device = (lax.select(side == 0, along_x(-1)[0], along_x(1)[0]), gz)
        plan = []
        both = (2, rows["both_from"], rows["both_to"])
        near = (1, rows["near_from"], rows["to_halo"])
        far = (1, rows["far_from"], rows["to_far"])
        for ks in (pl.ds(0, 2), pl.ds(nz - 2, 2)):
            plan.append((*both, ks, pl.ds(0, ny)))
        for ks in inner:
            plan.append((*near, ks, pl.ds(0, ny)))
        for cols in tiles:
            for ks in inner:
                plan.append((*far, ks, cols))
        return [remote(pad.at[:, pl.ds(src, deep), ks, cols], pad.at[:, pl.ds(dst, deep), ks, cols],
                       xs_sem, xr_sem.at[group_of(n)], device)
                for n, (deep, src, dst, ks, cols) in enumerate(plan)]

    pieces = [x_pieces(p) for p in range(2)]
    detour = gxn >= 4 and gxn % 2 == 0
    odd = parity == 1
    sends_via = (odd & (gx < gxn - 1)) | (gx == 0)
    carries = (jnp.logical_not(odd) & (gx < gxn - 2)) | (gx == 1)
    partner = lax.select(odd, along_x(-1)[0], along_x(1)[0])
    beyond = lax.select(odd, along_x(-2)[0], along_x(2)[0])
    via = [remote(pad.at[:, pl.ds(sides[0]["far_from"], 1), ks, tiles[-1]], via_ref.at[:, :, ks],
                  xs_sem, via_sem.at[0], (partner, gz)) for ks in inner]
    onward = [remote(via_ref.at[:, :, ks], pad.at[:, pl.ds(lax.select(odd, nx + 3, 0), 1), ks, tiles[-1]],
                     via_sem.at[1], xr_sem.at[1 + len(tiles)], (beyond, gz)) for ks in inner]
    k_up = remote(pad.at[:, 2:nx + 2, nz - 2:nz], pad.at[:, 2:nx + 2, wide - 2:wide], ks_sem, kr_sem, along_z(1))
    k_down = remote(pad.at[:, 2:nx + 2, 0:2], pad.at[:, 2:nx + 2, nz:nz + 2], ks_sem, kr_sem, along_z(-1))

    def far(t):
        return tuple(range(5 + 3 * t, 8 + 3 * t))

    def wait_for(columns, sem, cols=pl.ds(0, ny)):
        ref = pad.at[:, 0:columns // 8, 0:8, cols]
        remote(ref, ref, sem, sem, (gx, gz)).wait_recv()

    def send(*which, sides=(0, 1)):
        for n in which:
            for p in sides:
                if detour and p == 0 and n in far(len(tiles) - 1):
                    pl.when(jnp.logical_not(sends_via))(pieces[p][n].start)
                else:
                    pieces[p][n].start()

    def send_via():
        if detour:
            @pl.when(sends_via)
            def _():
                for copy in via:
                    copy.start()

    def send_onward():
        if detour:
            @pl.when(carries)
            def _():
                remote(count_ref, count_ref, via_sem.at[0], via_sem.at[0], (gx, gz)).wait_recv()
                for copy in onward:
                    copy.start()

    pltpu.make_async_copy(vel_ref.at[:, 0:4], pad.at[:, 0:4, 0:nz], load_sem.at[0]).wait()
    pl.semaphore_wait(barrier, 3 + behind.astype(jnp.int32))

    @pl.when(jnp.logical_not(ahead))
    def _():
        signal(wrap_sem, along_x(1))

    send(*EDGES, *NEAR, sides=(1,))

    @pl.when(behind)
    def _():
        send(*EDGES, *NEAR, sides=(0,))

    loads[2].wait()
    k_up.start()
    k_down.start()

    know_x, know_z = doublings(gxn), doublings(gzn)
    direct = gxn * gzn <= DIRECT

    def learn_steps():
        last = max(len(know_x), len(know_z))
        for j in range(last + 1):
            if j > 0:
                for sem, steps in ((near_x, know_x), (near_z, know_z)):
                    if j <= len(steps):
                        pl.semaphore_wait(sem.at[j - 1], 2)
            for sem, steps, along in ((near_x, know_x, along_x), (near_z, know_z, along_z)):
                if j < len(steps):
                    signal(sem.at[j], along(steps[j]))
                    signal(sem.at[j], along(-steps[j]))
            if j < last:
                yield
        if direct and gzn > 1:
            for d in range(1, gzn):
                signal(near_all, along_z(d))
            yield
            pl.semaphore_wait(near_all, gzn - 1)

    steps = learn_steps()

    def learn():
        next(steps, None)

    sums[...] = jnp.zeros_like(sums)
    gap_load.wait()
    span = gap_ref[:, 0:ny] + gap_ref[:, 1:ny + 1]
    at = lax.broadcasted_iota(jnp.int32, (1, ny), 1)
    width_sq = width_square(span)
    inverse = 2.0 / span
    coef_ref[0:1] = jnp.where(at == ny - 1, 0.0, inverse)
    coef_ref[1:2] = jnp.where(at == 0, 0.0, inverse)
    coef_ref[2:3] = width_sq * (1.0 / 256.0)
    coef_ref[3:4] = width_sq * width_sq * (1.0 / 256.0)
    coef_ref[4:5] = width_sq
    half_ahead, half_back = coef_ref[0:1, :], coef_ref[1:2, :]

    def filtered(f):
        twice = f + pltpu.roll(f, 1, 0)
        return twice + pltpu.roll(twice, wide - 1, 0)

    def lane_slope(f):
        return pltpu.roll(f, ny - 1, 1) * half_ahead - pltpu.roll(f, 1, 1) * half_back

    def smooth_tile(r, cols):
        for c in range(3):
            zvel[c, r, :, cols] = filtered(pad[c, r, :, cols])

    def smooth_row(r):
        for cols in tiles:
            smooth_tile(r, cols)

    def first_slope(r):
        for c in range(3):
            slope[c] = lane_slope(pad[c, r])

    def strain_size(f):
        square = [s * s for s in f]
        return jnp.sqrt(0.5 * (square[0] + square[1] + square[2]) + 0.25 * (square[3] + square[4] + square[5]))

    def stress_tile(r, cols):
        u = [pad[c, r, :, cols] for c in range(3)]
        a = [pad[c, r + 1, :, cols] - pad[c, r - 1, :, cols] for c in range(3)]
        b = []
        for c in range(3):
            prev, nxt = pltpu.roll(u[c], 1, 0), pltpu.roll(u[c], wide - 1, 0)
            b.append(nxt - prev)
            zvel[c, r, :, cols] = (nxt + prev) + 2.0 * u[c]
        d = [slope[c, :, cols] for c in range(3)]
        strain = [a[0], d[1], b[2], d[0] + a[1], b[0] + a[2], b[1] + d[2]]
        size = strain_size(strain)
        size_s[r - 2, :, cols] = size[:nz]
        for n in range(6):
            zstress[n, r, :, cols] = filtered(size * strain[n])[:nz]

    def pair_tile(r, cols):
        u = [pad[c, r, :, cols] for c in range(3)]
        for n, (i, j) in enumerate(PAIRS):
            zpair[n, r, :, cols] = filtered(u[i] * u[j])[:nz]

    def first(r):
        first_slope(r)
        for cols in tiles:
            stress_tile(r, cols)
            pair_tile(r, cols)

    def second_slope(r):
        for c in range(3):
            v = (zvel[c, r - 1] + zvel[c, r + 1]) + 2.0 * zvel[c, r]
            tslope[c] = v
            vslope[c] = lane_slope(v)

    def leonard(r, cols):
        v = [tslope[c, 0:nz, cols] for c in range(3)]
        out = []
        for n, (i, j) in enumerate(PAIRS):
            pair = (zpair[n, r - 1, :, cols] + zpair[n, r + 1, :, cols]) + 2.0 * zpair[n, r, :, cols]
            out.append(pair - v[i] * v[j] * 0.0625)
        return out

    def contract(r, cols, test, stress, leon):
        w = coef_ref[2:3, cols]
        w2 = coef_ref[3:4, cols]
        q = 0.25 * strain_size(test)
        lm, mm_diag, mm_off = 0.0, 0.0, 0.0
        for n in range(6):
            model = stress[n] - q * test[n]
            lm = lm + leon[n] * model
            if n < 3:
                mm_diag = mm_diag + model * model
            else:
                mm_off = mm_off + model * model
        lm = lm * w
        mm = (mm_diag + 0.5 * mm_off) * w2
        lm_s[r - 2, :, cols] = lm
        mm_s[r - 2, :, cols] = mm
        for n, f in enumerate((lm, mm)):
            sums[n, :, cols] += jnp.sum(f.reshape(nz // 8, 8, LANES), axis=0)

    def second_tile(r, cols):
        v_wide = [tslope[c, :, cols] for c in range(3)]
        a = [(zvel[c, r + 2, 0:nz, cols] - zvel[c, r - 2, 0:nz, cols])
             + 2.0 * (zvel[c, r + 1, 0:nz, cols] - zvel[c, r - 1, 0:nz, cols]) for c in range(3)]
        b = [(pltpu.roll(f, wide - 1, 0) - pltpu.roll(f, 1, 0))[:nz] for f in v_wide]
        d = [vslope[c, 0:nz, cols] for c in range(3)]
        test = [a[0], d[1], b[2], d[0] + a[1], b[0] + a[2], b[1] + d[2]]
        stress = [(zstress[n, r - 1, :, cols] + zstress[n, r + 1, :, cols]) + 2.0 * zstress[n, r, :, cols] for n in range(6)]
        contract(r, cols, test, stress, leonard(r, cols))

    def second(r):
        second_slope(r)
        for cols in tiles:
            second_tile(r, cols)

    def over(lo, hi, body):
        def step(r, carry):
            body(r)
            return carry
        lax.fori_loop(lo, hi, step, 0)


    @pl.when(jnp.logical_not(behind))
    def _():
        pl.semaphore_wait(wrap_sem, 1)
        send(*EDGES, *NEAR, sides=(0,))

    learn()
    wait_for(4 * nx, kr_sem)
    over(3, nx + 1, first)
    learn()
    send_via()
    smooth_row(2)
    smooth_row(nx + 1)
    over(4, nx, second)
    send(*far(0))
    send(*far(1))
    send(*far(2))
    wait_for(16, xr_sem.at[0])
    relayed = []
    for p in range(2):
        rows = pl.ds(sides[p]["both"], 2)
        for n, (src, dst, device) in enumerate(((nz - 2, wide - 2, along_z(1)), (0, nz, along_z(-1)))):
            relayed.append(remote(pad.at[:, rows, pl.ds(src, 2)], pad.at[:, rows, pl.ds(dst, 2)], cs_sem, cr_sem, device))
    for copy in relayed:
        copy.start()

    def both(body):
        for p in range(2):
            body(p, sides[p])

    wait_for(2 * (nz - 4), xr_sem.at[1])
    learn()
    wait_for(16, cr_sem)
    send_onward()

    def ready(p, rows):
        halo, edge = rows["halo"], rows["edge"]
        first(edge)
        smooth_row(halo)
        second(rows["inner"])
        first_slope(halo)
        second_slope(edge)
        for cols in tiles:
            pair_tile(halo, cols)
            u = [pad[c, halo, :, cols] for c in range(3)]
            b = [pltpu.roll(f, wide - 1, 0) - pltpu.roll(f, 1, 0) for f in u]
            d = [slope[c, :, cols] for c in range(3)]
            for n, f in enumerate((d[1], b[2], d[0], b[0], b[1] + d[2])):
                strain_ref[p, n, :, cols] = f
            v = [tslope[c, :, cols] for c in range(3)]
            b = [(pltpu.roll(f, wide - 1, 0) - pltpu.roll(f, 1, 0))[:nz] for f in v]
            a = [signs[p] * zvel[c, rows["other"], 0:nz, cols] + 2.0 * (zvel[c, edge + 1, 0:nz, cols] - zvel[c, edge - 1, 0:nz, cols])
                 for c in range(3)]
            d = [vslope[c, 0:nz, cols] for c in range(3)]
            leon = leonard(edge, cols)
            for n, f in enumerate((a[0], d[1], b[2], d[0] + a[1], b[0] + a[2], b[1] + d[2])):
                test_ref[p, n, :, cols] = f
                leon_ref[p, n, :, cols] = leon[n]
                rest_ref[p, n, :, cols] = zstress[n, rows["inner"], :, cols] + 2.0 * zstress[n, edge, :, cols]

    ready(0, sides[0])
    ready(1, sides[1])
    for _ in steps:
        pass
    here = gx * gzn + gz
    if direct:
        rounds = [(here, [(ox, oz) for ox in range(gxn) for oz in range(gzn)], gxn * gzn - 1)]
    else:
        rounds = [(gz, [(gx, oz) for oz in range(gzn)], gzn - 1), (gx, [(ox, gz) for ox in range(gxn)], gxn - 1)]

    def spread(n, t, value):
        slot, devices, _ = rounds[n]
        acc = accs[n].at[t]
        acc[slot] = value
        for device in devices:
            @pl.when((device[0] != gx) | (device[1] != gz))
            def _():
                remote(acc.at[slot], acc.at[slot], as_sem.at[n], ar_sem.at[n, t], device).start()

    def gathered(n, t):
        acc, count = accs[n].at[t], rounds[n][2]
        return remote(acc.at[0:count], acc.at[0:count], as_sem.at[n], ar_sem.at[n, t], (gx, gz))

    for t, cols in enumerate(tiles):
        wait_for(2 * (nz - 4), xr_sem.at[2 + t], tiles[0])

        def finish_rows(p, rows):
            u = [pad[c, rows["far"], :, cols] for c in range(3)]
            a = [signs[p] * (pad[c, rows["edge"], :, cols] - u[c]) for c in range(3)]
            part = [strain_ref[p, n, :, cols] for n in range(5)]
            strain = [a[0], part[0], part[1], part[2] + a[1], part[3] + a[2], part[4]]
            size = strain_size(strain)
            part = [test_ref[p, n, :, cols] for n in range(6)]
            a = [signs[p] * filtered(f)[:nz] for f in u]
            test = [part[0] - a[0], part[1], part[2], part[3] - a[1], part[4] - a[2], part[5]]
            stress = [rest_ref[p, n, :, cols] + filtered(size * strain[n])[:nz] for n in range(6)]
            contract(rows["edge"], cols, test, stress, [leon_ref[p, n, :, cols] for n in range(6)])

        both(finish_rows)
        spread(0, t, jnp.sum(sums[:, :, cols], axis=1))
    for n in range(1, len(rounds) + 1):
        for t, cols in enumerate(tiles):
            gathered(n - 1, t).wait_recv()
            total = jnp.sum(accs[n - 1][t], axis=0)
            if n < len(rounds):
                spread(n, t, total)
            else:
                coefficient = total[0:1] / cells / (total[1:2] / cells + 1e-06)
                out_coef_ref[0:1, cols] = coefficient
                out_coef_ref[1:2, cols] = coefficient * coef_ref[4:5, cols]
    wait_for(4 * nx, ks_sem)
    block = pad.at[:, 0:4, 0:nz]
    remote(block, block, xs_sem, xs_sem, (gx, gz)).wait_send()
    wait_for(16, cs_sem)
    if detour:
        @pl.when(carries)
        def _():
            remote(count_ref, count_ref, via_sem.at[1], via_sem.at[1], (gx, gz)).wait_send()
    for n, (_, _, count) in enumerate(rounds):
        acc = accs[n].at[:, 0:count]
        remote(acc, acc, as_sem.at[n], as_sem.at[n], (gx, gz)).wait_send()


def per_device(velocity, y_gap):
    gxn, gzn = lax.axis_size("gx"), lax.axis_size("gz")
    _, nx, nz, ny = velocity.shape
    cells = float(nx * gxn * nz * gzn)
    field = jax.ShapeDtypeStruct((nx, nz, ny), jnp.float32)
    f32 = jnp.float32
    wide = nz + RIM
    dma, flag = pltpu.SemaphoreType.DMA, pltpu.SemaphoreType.REGULAR
    members = (gxn * gzn,) if gxn * gzn <= DIRECT else (gzn, gxn)
    gaps = y_gap.reshape(1, ny + 1)
    near = pl.BlockSpec(memory_space=pltpu.VMEM)
    far = pl.BlockSpec(memory_space=pl.ANY)
    held = pltpu.VMEM((nx, nz, ny), f32)
    size, lm, mm, coefficient = pl.pallas_call(
        functools.partial(kernel, gxn, gzn, cells),
        out_shape=(held, held, held, pltpu.VMEM((2, ny), f32)),
        in_specs=[far, far],
        out_specs=(near,) * 4,
        scratch_shapes=[
            pltpu.VMEM((3, nx + 4, wide, ny), f32),
            pltpu.VMEM((3, nx + 4, wide, ny), f32),
            pltpu.VMEM((6, nx + 4, nz, ny), f32),
            pltpu.VMEM((6, nx + 4, nz, ny), f32),
            pltpu.VMEM((3, wide, ny), f32),
            pltpu.VMEM((3, wide, ny), f32),
            pltpu.VMEM((3, wide, ny), f32),
            pltpu.VMEM((2, 5, wide, ny), f32),
            pltpu.VMEM((2, 6, nz, ny), f32),
            pltpu.VMEM((2, 6, nz, ny), f32),
            pltpu.VMEM((2, 6, nz, ny), f32),
            pltpu.VMEM((8, ny), f32),
            pltpu.VMEM((2, 8, ny), f32),
            tuple(pltpu.VMEM((ny // LANES, n, 2, LANES), f32) for n in members),
            pltpu.VMEM((3, 1, nz, LANES), f32), pltpu.VMEM((3 * (nz - 4) // 4, 4, LANES), f32),
            pltpu.VMEM((1, ny + 1), f32), dma,
            dma((2,)), dma, dma((2 + ny // LANES,)), dma, dma, dma, dma,
            flag((max(len(doublings(gxn)), 1),)), flag((max(len(doublings(gzn)), 1),)), flag, flag, dma((2,)),
            dma((len(members),)), dma((len(members), ny // LANES)),
        ],
        compiler_params=pltpu.CompilerParams(
            collective_id=0, has_side_effects=True, vmem_limit_bytes=40 * 2**20),
    )(pltpu.with_memory_space_constraint(gaps, pltpu.HBM), pltpu.with_memory_space_constraint(velocity, pltpu.HBM))
    return pl.pallas_call(
        finish,
        out_shape=(field, field, field, jax.ShapeDtypeStruct((ny,), f32)),
        in_specs=[near] * 4,
        out_specs=(far,) * 4,
        scratch_shapes=[pltpu.VMEM((nx, nz, ny), f32), pltpu.VMEM((ny,), f32), dma((4,))],
        compiler_params=pltpu.CompilerParams(vmem_limit_bytes=8 * 2**20),
    )(size, lm, mm, coefficient)


def solution(mesh):
    placed = (P(None, "gx", "gz", None), P())
    return jax.shard_map(
        per_device,
        mesh=mesh,
        in_specs=placed,
        out_specs=(P("gx", "gz", None), P("gx", "gz", None), P("gx", "gz", None), P()),
        check_vma=False,
    )
```

```python
import functools

import jax
import jax.numpy as jnp
from jax import lax
from jax.experimental import pallas as pl
from jax.experimental.pallas import tpu as pltpu
from jax.sharding import PartitionSpec as P

MESH = pl.DeviceIdType.MESH
LANES = 128
RIM = 8
DIRECT = 64
EDGES, NEAR = (0, 1), (2, 3, 4)
PAIRS = ((0, 0), (1, 1), (2, 2), (0, 1), (0, 2), (1, 2))


def width_square(span):
    return jnp.exp(jnp.log(0.5 * span) * (2.0 / 3.0))


def finish(size_ref, lm_ref, mm_ref, coef_ref, eddy_out, lm_out, mm_out, coef_out, eddy_s, coef_s, sem):
    nx = size_ref.shape[0]
    copies = [pltpu.make_async_copy(lm_ref, lm_out, sem.at[0]), pltpu.make_async_copy(mm_ref, mm_out, sem.at[1])]
    coef_s[...] = coef_ref[0:1].reshape(coef_s.shape)
    copies.append(pltpu.make_async_copy(coef_s, coef_out, sem.at[2]))
    for copy in copies:
        copy.start()
    factor = coef_ref[1:2]
    for r in range(0, nx, 2):
        rows = pl.ds(r, 2)
        eddy_s[rows] = factor * size_ref[rows]
        pltpu.make_async_copy(eddy_s.at[rows], eddy_out.at[rows], sem.at[3]).start()
    copies.append(pltpu.make_async_copy(eddy_s, eddy_out, sem.at[3]))
    for copy in copies:
        copy.wait()


def doublings(size):
    reach, steps = 1, []
    while reach < size // 2:
        steps.append(reach)
        reach *= 2
    return steps


def kernel(gxn, gzn, cells, gap_hbm, vel_ref, size_s, lm_s, mm_s, out_coef_ref,
           pad, zvel, zpair, zstress, slope, tslope, vslope, strain_ref, test_ref, rest_ref, leon_ref, coef_ref, sums, accs, via_ref, count_ref,
           gap_ref, gap_sem, load_sem, xs_sem, xr_sem, ks_sem, kr_sem, cs_sem, cr_sem,
           near_x, near_z, near_all, wrap_sem, via_sem, as_sem, ar_sem):
    gx, gz = lax.axis_index("gx"), lax.axis_index("gz")
    nx, nz, ny = vel_ref.shape[1:]
    wide = nz + RIM
    tiles = [pl.ds(t, LANES) for t in range(0, ny, LANES)]

    def along_x(d):
        return (lax.rem(gx + d + gxn, gxn), gz)

    def along_z(d):
        return (gx, lax.rem(gz + d + gzn, gzn))

    def signal(sem, device):
        pl.semaphore_signal(sem, inc=1, device_id=device, device_id_type=MESH)

    def remote(src, dst, send, recv, device):
        return pltpu.make_async_remote_copy(
            src_ref=src, dst_ref=dst, send_sem=send, recv_sem=recv,
            device_id=device, device_id_type=MESH)

    barrier = pltpu.get_barrier_semaphore()
    for device in (along_x(-1), along_z(1), along_z(-1)):
        signal(barrier, device)
    ahead, behind = gx < gxn - 1, gx > 0

    @pl.when(ahead)
    def _():
        signal(barrier, along_x(1))

    loads = []
    for n, (lo, hi) in enumerate(((0, 2), (nx - 2, nx), (2, nx - 2))):
        loads.append(pltpu.make_async_copy(vel_ref.at[:, lo:hi], pad.at[:, lo + 2:hi + 2, 0:nz], load_sem.at[n // 2]))
    for load in loads:
        load.start()
    gap_load = pltpu.make_async_copy(gap_hbm, gap_ref, gap_sem)
    gap_load.start()

    def side_rows(side):
        def pick(low, high):
            return lax.select(side == 0, low, high)
        return dict(
            other=pick(4, nx - 1), inner=pick(3, nx), edge=pick(2, nx + 1), halo=pick(1, nx + 2), far=pick(0, nx + 3),
            to_halo=pick(nx + 2, 1), to_far=pick(nx + 3, 0), near_from=pick(2, nx + 1), far_from=pick(3, nx),
            both_from=pick(2, nx), both_to=pick(nx + 2, 0), both=pick(0, nx + 2))

    parity = lax.rem(gx, 2)
    order = (parity, 1 - parity)
    sides = [side_rows(side) for side in order]
    signs = [lax.select(side == 0, 1.0, -1.0) for side in order]

    def group_of(n):
        return 0 if n in EDGES else 1 if n in NEAR else 2 + (n - 5) // 3

    inner = (pl.ds(2, 6), pl.ds(8, nz - 16), pl.ds(nz - 8, 6))

    def x_pieces(p):
        side, rows = order[p], sides[p]
        device = (lax.select(side == 0, along_x(-1)[0], along_x(1)[0]), gz)
        plan = []
        both = (2, rows["both_from"], rows["both_to"])
        near = (1, rows["near_from"], rows["to_halo"])
        far = (1, rows["far_from"], rows["to_far"])
        for ks in (pl.ds(0, 2), pl.ds(nz - 2, 2)):
            plan.append((*both, ks, pl.ds(0, ny)))
        for ks in inner:
            plan.append((*near, ks, pl.ds(0, ny)))
        for cols in tiles:
            for ks in inner:
                plan.append((*far, ks, cols))
        return [remote(pad.at[:, pl.ds(src, deep), ks, cols], pad.at[:, pl.ds(dst, deep), ks, cols],
                       xs_sem, xr_sem.at[group_of(n)], device)
                for n, (deep, src, dst, ks, cols) in enumerate(plan)]

    pieces = [x_pieces(p) for p in range(2)]
    detour = gxn >= 4 and gxn % 2 == 0
    odd = parity == 1
    sends_via = (odd & (gx < gxn - 1)) | (gx == 0)
    carries = (jnp.logical_not(odd) & (gx < gxn - 2)) | (gx == 1)
    partner = lax.select(odd, along_x(-1)[0], along_x(1)[0])
    beyond = lax.select(odd, along_x(-2)[0], along_x(2)[0])
    via = [remote(pad.at[:, pl.ds(sides[0]["far_from"], 1), ks, tiles[-1]], via_ref.at[:, :, ks],
                  xs_sem, via_sem.at[0], (partner, gz)) for ks in inner]
    onward = [remote(via_ref.at[:, :, ks], pad.at[:, pl.ds(lax.select(odd, nx + 3, 0), 1), ks, tiles[-1]],
                     via_sem.at[1], xr_sem.at[1 + len(tiles)], (beyond, gz)) for ks in inner]
    k_up = remote(pad.at[:, 2:nx + 2, nz - 2:nz], pad.at[:, 2:nx + 2, wide - 2:wide], ks_sem, kr_sem, along_z(1))
    k_down = remote(pad.at[:, 2:nx + 2, 0:2], pad.at[:, 2:nx + 2, nz:nz + 2], ks_sem, kr_sem, along_z(-1))

    def far(t):
        return tuple(range(5 + 3 * t, 8 + 3 * t))

    def wait_for(columns, sem, cols=pl.ds(0, ny)):
        ref = pad.at[:, 0:columns // 8, 0:8, cols]
        remote(ref, ref, sem, sem, (gx, gz)).wait_recv()

    def send(*which, sides=(0, 1)):
        for n in which:
            for p in sides:
                if detour and p == 0 and n in far(len(tiles) - 1):
                    pl.when(jnp.logical_not(sends_via))(pieces[p][n].start)
                else:
                    pieces[p][n].start()

    def send_via():
        if detour:
            @pl.when(sends_via)
            def _():
                for copy in via:
                    copy.start()

    def send_onward():
        if detour:
            @pl.when(carries)
            def _():
                remote(count_ref, count_ref, via_sem.at[0], via_sem.at[0], (gx, gz)).wait_recv()
                for copy in onward:
                    copy.start()

    pltpu.make_async_copy(vel_ref.at[:, 0:4], pad.at[:, 0:4, 0:nz], load_sem.at[0]).wait()
    pl.semaphore_wait(barrier, 3 + behind.astype(jnp.int32))

    @pl.when(jnp.logical_not(ahead))
    def _():
        signal(wrap_sem, along_x(1))

    send(*EDGES, *NEAR, sides=(1,))

    @pl.when(behind)
    def _():
        send(*EDGES, *NEAR, sides=(0,))

    loads[2].wait()
    k_up.start()
    k_down.start()

    know_x, know_z = doublings(gxn), doublings(gzn)
    direct = gxn * gzn <= DIRECT

    def learn_steps():
        last = max(len(know_x), len(know_z))
        for j in range(last + 1):
            if j > 0:
                for sem, steps in ((near_x, know_x), (near_z, know_z)):
                    if j <= len(steps):
                        pl.semaphore_wait(sem.at[j - 1], 2)
            for sem, steps, along in ((near_x, know_x, along_x), (near_z, know_z, along_z)):
                if j < len(steps):
                    signal(sem.at[j], along(steps[j]))
                    signal(sem.at[j], along(-steps[j]))
            if j < last:
                yield
        if direct and gzn > 1:
            for d in range(1, gzn):
                signal(near_all, along_z(d))
            yield
            pl.semaphore_wait(near_all, gzn - 1)

    steps = learn_steps()

    def learn():
        next(steps, None)

    sums[...] = jnp.zeros_like(sums)
    gap_load.wait()
    span = gap_ref[:, 0:ny] + gap_ref[:, 1:ny + 1]
    at = lax.broadcasted_iota(jnp.int32, (1, ny), 1)
    width_sq = width_square(span)
    inverse = 2.0 / span
    coef_ref[0:1] = jnp.where(at == ny - 1, 0.0, inverse)
    coef_ref[1:2] = jnp.where(at == 0, 0.0, inverse)
    coef_ref[2:3] = width_sq * (1.0 / 256.0)
    coef_ref[3:4] = width_sq * width_sq * (1.0 / 256.0)
    coef_ref[4:5] = width_sq
    half_ahead, half_back = coef_ref[0:1, :], coef_ref[1:2, :]

    def filtered(f):
        twice = f + pltpu.roll(f, 1, 0)
        return twice + pltpu.roll(twice, wide - 1, 0)

    def lane_slope(f):
        return pltpu.roll(f, ny - 1, 1) * half_ahead - pltpu.roll(f, 1, 1) * half_back

    def smooth_tile(r, cols):
        for c in range(3):
            zvel[c, r, :, cols] = filtered(pad[c, r, :, cols])

    def smooth_row(r):
        for cols in tiles:
            smooth_tile(r, cols)

    def first_slope(r):
        for c in range(3):
            slope[c] = lane_slope(pad[c, r])

    def strain_size(f):
        square = [s * s for s in f]
        return jnp.sqrt(0.5 * (square[0] + square[1] + square[2]) + 0.25 * (square[3] + square[4] + square[5]))

    def stress_tile(r, cols):
        u = [pad[c, r, :, cols] for c in range(3)]
        a = [pad[c, r + 1, :, cols] - pad[c, r - 1, :, cols] for c in range(3)]
        b = []
        for c in range(3):
            prev, nxt = pltpu.roll(u[c], 1, 0), pltpu.roll(u[c], wide - 1, 0)
            b.append(nxt - prev)
            zvel[c, r, :, cols] = (nxt + prev) + 2.0 * u[c]
        d = [slope[c, :, cols] for c in range(3)]
        strain = [a[0], d[1], b[2], d[0] + a[1], b[0] + a[2], b[1] + d[2]]
        size = strain_size(strain)
        size_s[r - 2, :, cols] = size[:nz]
        for n in range(6):
            zstress[n, r, :, cols] = filtered(size * strain[n])[:nz]

    def pair_tile(r, cols):
        u = [pad[c, r, :, cols] for c in range(3)]
        for n, (i, j) in enumerate(PAIRS):
            zpair[n, r, :, cols] = filtered(u[i] * u[j])[:nz]

    def first(r):
        first_slope(r)
        for cols in tiles:
            stress_tile(r, cols)
            pair_tile(r, cols)

    def second_slope(r):
        for c in range(3):
            v = (zvel[c, r - 1] + zvel[c, r + 1]) + 2.0 * zvel[c, r]
            tslope[c] = v
            vslope[c] = lane_slope(v)

    def leonard(r, cols):
        v = [tslope[c, 0:nz, cols] for c in range(3)]
        out = []
        for n, (i, j) in enumerate(PAIRS):
            pair = (zpair[n, r - 1, :, cols] + zpair[n, r + 1, :, cols]) + 2.0 * zpair[n, r, :, cols]
            out.append(pair - v[i] * v[j] * 0.0625)
        return out

    def contract(r, cols, test, stress, leon):
        w = coef_ref[2:3, cols]
        w2 = coef_ref[3:4, cols]
        q = 0.25 * strain_size(test)
        lm, mm_diag, mm_off = 0.0, 0.0, 0.0
        for n in range(6):
            model = stress[n] - q * test[n]
            lm = lm + leon[n] * model
            if n < 3:
                mm_diag = mm_diag + model * model
            else:
                mm_off = mm_off + model * model
        lm = lm * w
        mm = (mm_diag + 0.5 * mm_off) * w2
        lm_s[r - 2, :, cols] = lm
        mm_s[r - 2, :, cols] = mm
        for n, f in enumerate((lm, mm)):
            sums[n, :, cols] += jnp.sum(f.reshape(nz // 8, 8, LANES), axis=0)

    def second_tile(r, cols):
        v_wide = [tslope[c, :, cols] for c in range(3)]
        a = [(zvel[c, r + 2, 0:nz, cols] - zvel[c, r - 2, 0:nz, cols])
             + 2.0 * (zvel[c, r + 1, 0:nz, cols] - zvel[c, r - 1, 0:nz, cols]) for c in range(3)]
        b = [(pltpu.roll(f, wide - 1, 0) - pltpu.roll(f, 1, 0))[:nz] for f in v_wide]
        d = [vslope[c, 0:nz, cols] for c in range(3)]
        test = [a[0], d[1], b[2], d[0] + a[1], b[0] + a[2], b[1] + d[2]]
        stress = [(zstress[n, r - 1, :, cols] + zstress[n, r + 1, :, cols]) + 2.0 * zstress[n, r, :, cols] for n in range(6)]
        contract(r, cols, test, stress, leonard(r, cols))

    def second(r):
        second_slope(r)
        for cols in tiles:
            second_tile(r, cols)

    def over(lo, hi, body):
        def step(r, carry):
            body(r)
            return carry
        lax.fori_loop(lo, hi, step, 0)


    @pl.when(jnp.logical_not(behind))
    def _():
        pl.semaphore_wait(wrap_sem, 1)
        send(*EDGES, *NEAR, sides=(0,))

    learn()
    wait_for(4 * nx, kr_sem)
    over(3, nx + 1, first)
    learn()
    send_via()
    smooth_row(2)
    smooth_row(nx + 1)
    over(4, nx, second)
    wait_for(16, xr_sem.at[0])
    relayed = []
    for p in range(2):
        rows = pl.ds(sides[p]["both"], 2)
        for n, (src, dst, device) in enumerate(((nz - 2, wide - 2, along_z(1)), (0, nz, along_z(-1)))):
            relayed.append(remote(pad.at[:, rows, pl.ds(src, 2)], pad.at[:, rows, pl.ds(dst, 2)], cs_sem, cr_sem, device))
    for copy in relayed:
        copy.start()
    send(*far(0))
    send(*far(1))
    send(*far(2))

    def both(body):
        for p in range(2):
            body(p, sides[p])

    wait_for(2 * (nz - 4), xr_sem.at[1])
    learn()
    wait_for(16, cr_sem)

    def ready(p, rows):
        halo, edge = rows["halo"], rows["edge"]
        first(edge)
        smooth_row(halo)
        second(rows["inner"])
        first_slope(halo)
        second_slope(edge)
        for cols in tiles:
            pair_tile(halo, cols)
            u = [pad[c, halo, :, cols] for c in range(3)]
            b = [pltpu.roll(f, wide - 1, 0) - pltpu.roll(f, 1, 0) for f in u]
            d = [slope[c, :, cols] for c in range(3)]
            for n, f in enumerate((d[1], b[2], d[0], b[0], b[1] + d[2])):
                strain_ref[p, n, :, cols] = f
            v = [tslope[c, :, cols] for c in range(3)]
            b = [(pltpu.roll(f, wide - 1, 0) - pltpu.roll(f, 1, 0))[:nz] for f in v]
            a = [signs[p] * zvel[c, rows["other"], 0:nz, cols] + 2.0 * (zvel[c, edge + 1, 0:nz, cols] - zvel[c, edge - 1, 0:nz, cols])
                 for c in range(3)]
            d = [vslope[c, 0:nz, cols] for c in range(3)]
            leon = leonard(edge, cols)
            for n, f in enumerate((a[0], d[1], b[2], d[0] + a[1], b[0] + a[2], b[1] + d[2])):
                test_ref[p, n, :, cols] = f
                leon_ref[p, n, :, cols] = leon[n]
                rest_ref[p, n, :, cols] = zstress[n, rows["inner"], :, cols] + 2.0 * zstress[n, edge, :, cols]

    ready(0, sides[0])
    send_onward()
    ready(1, sides[1])
    for _ in steps:
        pass
    here = gx * gzn + gz
    if direct:
        rounds = [(here, [(ox, oz) for ox in range(gxn) for oz in range(gzn)], gxn * gzn - 1)]
    else:
        rounds = [(gz, [(gx, oz) for oz in range(gzn)], gzn - 1), (gx, [(ox, gz) for ox in range(gxn)], gxn - 1)]

    def spread(n, t, value):
        slot, devices, _ = rounds[n]
        acc = accs[n].at[t]
        acc[slot] = value
        for device in devices:
            @pl.when((device[0] != gx) | (device[1] != gz))
            def _():
                remote(acc.at[slot], acc.at[slot], as_sem.at[n], ar_sem.at[n, t], device).start()

    def gathered(n, t):
        acc, count = accs[n].at[t], rounds[n][2]
        return remote(acc.at[0:count], acc.at[0:count], as_sem.at[n], ar_sem.at[n, t], (gx, gz))

    for t, cols in enumerate(tiles):
        wait_for(2 * (nz - 4), xr_sem.at[2 + t], tiles[0])

        def finish_rows(p, rows):
            u = [pad[c, rows["far"], :, cols] for c in range(3)]
            a = [signs[p] * (pad[c, rows["edge"], :, cols] - u[c]) for c in range(3)]
            part = [strain_ref[p, n, :, cols] for n in range(5)]
            strain = [a[0], part[0], part[1], part[2] + a[1], part[3] + a[2], part[4]]
            size = strain_size(strain)
            part = [test_ref[p, n, :, cols] for n in range(6)]
            a = [signs[p] * filtered(f)[:nz] for f in u]
            test = [part[0] - a[0], part[1], part[2], part[3] - a[1], part[4] - a[2], part[5]]
            stress = [rest_ref[p, n, :, cols] + filtered(size * strain[n])[:nz] for n in range(6)]
            contract(rows["edge"], cols, test, stress, [leon_ref[p, n, :, cols] for n in range(6)])

        both(finish_rows)
        spread(0, t, jnp.sum(sums[:, :, cols], axis=1))
    for n in range(1, len(rounds) + 1):
        for t, cols in enumerate(tiles):
            gathered(n - 1, t).wait_recv()
            total = jnp.sum(accs[n - 1][t], axis=0)
            if n < len(rounds):
                spread(n, t, total)
            else:
                coefficient = total[0:1] / cells / (total[1:2] / cells + 1e-06)
                out_coef_ref[0:1, cols] = coefficient
                out_coef_ref[1:2, cols] = coefficient * coef_ref[4:5, cols]
    wait_for(4 * nx, ks_sem)
    block = pad.at[:, 0:4, 0:nz]
    remote(block, block, xs_sem, xs_sem, (gx, gz)).wait_send()
    wait_for(16, cs_sem)
    if detour:
        @pl.when(carries)
        def _():
            remote(count_ref, count_ref, via_sem.at[1], via_sem.at[1], (gx, gz)).wait_send()
    for n, (_, _, count) in enumerate(rounds):
        acc = accs[n].at[:, 0:count]
        remote(acc, acc, as_sem.at[n], as_sem.at[n], (gx, gz)).wait_send()


def per_device(velocity, y_gap):
    gxn, gzn = lax.axis_size("gx"), lax.axis_size("gz")
    _, nx, nz, ny = velocity.shape
    cells = float(nx * gxn * nz * gzn)
    field = jax.ShapeDtypeStruct((nx, nz, ny), jnp.float32)
    f32 = jnp.float32
    wide = nz + RIM
    dma, flag = pltpu.SemaphoreType.DMA, pltpu.SemaphoreType.REGULAR
    members = (gxn * gzn,) if gxn * gzn <= DIRECT else (gzn, gxn)
    gaps = y_gap.reshape(1, ny + 1)
    near = pl.BlockSpec(memory_space=pltpu.VMEM)
    far = pl.BlockSpec(memory_space=pl.ANY)
    held = pltpu.VMEM((nx, nz, ny), f32)
    size, lm, mm, coefficient = pl.pallas_call(
        functools.partial(kernel, gxn, gzn, cells),
        out_shape=(held, held, held, pltpu.VMEM((2, ny), f32)),
        in_specs=[far, far],
        out_specs=(near,) * 4,
        scratch_shapes=[
            pltpu.VMEM((3, nx + 4, wide, ny), f32),
            pltpu.VMEM((3, nx + 4, wide, ny), f32),
            pltpu.VMEM((6, nx + 4, nz, ny), f32),
            pltpu.VMEM((6, nx + 4, nz, ny), f32),
            pltpu.VMEM((3, wide, ny), f32),
            pltpu.VMEM((3, wide, ny), f32),
            pltpu.VMEM((3, wide, ny), f32),
            pltpu.VMEM((2, 5, wide, ny), f32),
            pltpu.VMEM((2, 6, nz, ny), f32),
            pltpu.VMEM((2, 6, nz, ny), f32),
            pltpu.VMEM((2, 6, nz, ny), f32),
            pltpu.VMEM((8, ny), f32),
            pltpu.VMEM((2, 8, ny), f32),
            tuple(pltpu.VMEM((ny // LANES, n, 2, LANES), f32) for n in members),
            pltpu.VMEM((3, 1, nz, LANES), f32), pltpu.VMEM((3 * (nz - 4) // 4, 4, LANES), f32),
            pltpu.VMEM((1, ny + 1), f32), dma,
            dma((2,)), dma, dma((2 + ny // LANES,)), dma, dma, dma, dma,
            flag((max(len(doublings(gxn)), 1),)), flag((max(len(doublings(gzn)), 1),)), flag, flag, dma((2,)),
            dma((len(members),)), dma((len(members), ny // LANES)),
        ],
        compiler_params=pltpu.CompilerParams(
            collective_id=0, has_side_effects=True, vmem_limit_bytes=40 * 2**20),
    )(pltpu.with_memory_space_constraint(gaps, pltpu.HBM), pltpu.with_memory_space_constraint(velocity, pltpu.HBM))
    return pl.pallas_call(
        finish,
        out_shape=(field, field, field, jax.ShapeDtypeStruct((ny,), f32)),
        in_specs=[near] * 4,
        out_specs=(far,) * 4,
        scratch_shapes=[pltpu.VMEM((nx, nz, ny), f32), pltpu.VMEM((ny,), f32), dma((4,))],
        compiler_params=pltpu.CompilerParams(vmem_limit_bytes=8 * 2**20),
    )(size, lm, mm, coefficient)


def solution(mesh):
    placed = (P(None, "gx", "gz", None), P())
    return jax.shard_map(
        per_device,
        mesh=mesh,
        in_specs=placed,
        out_specs=(P("gx", "gz", None), P("gx", "gz", None), P("gx", "gz", None), P()),
        check_vma=False,
    )
```
